256 devices in a mesh: parts: 4 (over x, y), view: 64 (over z, core).
Axes of the slice: x: 2, y: 2, z: 32, core: 2. Of those that a mesh axis runs over, the one named last changes fastest.
The devices are a block of a 4x8x32 slice.
Arguments:
- volume: bfloat16 [32, 8, 128, 512], P(None, 'parts', 'view'), parts along dimension 1, may hold values from -6 to 6
- dual_state: bfloat16 [32, 8, 64, 512], P(None, 'parts', 'view'), parts along dimension 1, may hold values from -6 to 6
- sinogram: bfloat16 [4, 8, 64, 512], P(None, 'parts', 'view'), parts along dimension 1, may hold values from -6 to 6
- cot_volume: bfloat16 [32, 8, 128, 512], P(None, 'parts', 'view'), parts along dimension 1, may hold values from -6 to 6
- cot_dual: bfloat16 [32, 8, 64, 512], P(None, 'parts', 'view'), parts along dimension 1, may hold values from -6 to 6
- basis_table: bfloat16 [8, 32], replicated, may hold values from -1 to 1
- bin_energy: int32 [4], replicated, may hold values from 0 to 7
- footprint_table: bfloat16 [4, 1024, 128], replicated, may hold values from -0.0625 to 0.0625
- hit_tile: int32 [64, 48], replicated, may hold values from 0 to 63, as said below
- hit_table: int32 [64, 48], replicated, may hold values from 0 to 3
- hit_column: int32 [64, 48], replicated, may hold values from 0 to 3
- hit_count: int32 [64], replicated, may hold values from 8 to 48, as said below
- primal_inner: bfloat16 [27, 32, 36], replicated, may hold values from -0.1875 to 0.1875
- primal_inner_bias: float32 [32], replicated, may hold values from -3 to 3
- primal_outer: bfloat16 [27, 32, 32], replicated, may hold values from -0.21875 to 0.21875
- primal_outer_bias: float32 [32], replicated, may hold values from -3 to 3
- dual_inner: bfloat16 [27, 32, 40], replicated, may hold values from -0.1875 to 0.1875
- dual_inner_bias: float32 [32], replicated, may hold values from -3 to 3
- dual_outer: bfloat16 [27, 32, 32], replicated, may hold values from -0.21875 to 0.21875
- dual_outer_bias: float32 [32], replicated, may hold values from -3 to 3
Outputs:
- new_volume: bfloat16 [32, 8, 128, 512], P(None, 'parts', 'view'), parts along dimension 1
- new_dual: bfloat16 [32, 8, 64, 512], P(None, 'parts', 'view'), parts along dimension 1
- volume_grad: bfloat16 [32, 8, 128, 512], P(None, 'parts', 'view'), parts along dimension 1
- dual_grad: bfloat16 [32, 8, 64, 512], P(None, 'parts', 'view'), parts along dimension 1
- primal_inner_grad: float32 [108, 32, 36], P('parts'), parts along dimension 0
- primal_outer_grad: float32 [108, 32, 32], P('parts'), parts along dimension 0
- dual_inner_grad: float32 [108, 32, 40], P('parts'), parts along dimension 0
- dual_outer_grad: float32 [108, 32, 32], P('parts'), parts along dimension 0
The draws below stay inside these ranges and needn't reach their ends.
There are 4 independent parts, one for each index of `parts`. The reference program is written for one: setup_inputs(seed, part) draws one part's arguments, and reference() takes and returns one part's arrays. A program takes and returns all parts, laid end to end along the dimension named above; an argument that names none is the same for every part. Nothing has to cross between parts.
Inputs may be any that keep to these rules, and one draw needn't show every extreme that they name: `hit_tile`: each row holds 48 different tiles; a view block's rays cross the tiles of the first hit_count entries of its row. `hit_table`: only the live entries of a row matter. `hit_column`: only the live entries of a row matter. `hit_count`: some view block has exactly 48 live entries.
All inputs are finite; a program needn't handle non-finite values.
Results may differ from the reference program's by a relative error of at most 0.006.
Values may be sent and summed in bfloat16 or wider, within the bound.
A program may use at most 64 MiB of HBM per device.

```python
import jax
import jax.numpy as jnp
from jax import lax

C = 32
NB = 4
NE = 8
X = 512
U = 512
UW = 128
NOFF = 4
VB = 1
Z = 2
YT = 2
BLOCKS = 64
Y = 128
V = 64
K_MAX = 48


def draw_hit_tile(key, part):
    subkeys = jax.random.split(jax.random.fold_in(key, 11), BLOCKS)
    shuffled = jax.vmap(lambda subkey: jax.random.permutation(subkey, BLOCKS))(subkeys)
    return shuffled[:, :K_MAX].astype(jnp.int32)


def draw_hit_count(key, part):
    lowest = BLOCKS // 8
    counts_drawn = jax.random.randint(jax.random.fold_in(key, 23), (BLOCKS,), lowest, K_MAX + 1)
    fullest = jax.random.randint(jax.random.fold_in(key, 29), (), 0, BLOCKS)
    return jnp.where(jnp.arange(BLOCKS) == fullest, K_MAX, counts_drawn).astype(jnp.int32)


def with_ends(values, own_key, least, largest):
    longest = values.shape.index(max(values.shape))
    spots = []
    for shift in (0, 1):
        where = [jax.random.randint(jax.random.fold_in(own_key, axis), (), 0, length) for axis, length in enumerate(values.shape)]
        where[longest] = (where[longest] + shift) % values.shape[longest]
        spots.append(tuple(where))
    return values.at[spots[0]].set(least).at[spots[1]].set(largest)


def steps_of(rng, shape, cuts, least, largest):
    def one(position, shards_of):
        steps = jax.random.uniform(jax.random.fold_in(jax.random.fold_in(rng, 6), position), (shards_of,), jnp.float32, least / len(cuts), largest / len(cuts))
        return jnp.repeat(jnp.exp(steps), shape[position] // shards_of).reshape((-1,) + (1,) * (len(shape) - position - 1))

    factor_of = one(*cuts[0])
    for cut in cuts[1:]:
        factor_of = factor_of * one(*cut)
    return factor_of


def centred(rng, extent, scale, bound, pieces=(), kind=jnp.bfloat16):
    level = steps_of(rng, extent, pieces, -0.22, 0.18) if pieces else 1.0
    drawn = jax.random.normal(rng, extent, jnp.float32) * scale * level
    return jnp.minimum(jnp.maximum(drawn, -bound), bound).astype(kind)


def setup_inputs(seed: int = 0, part: int = 0) -> dict:
    key_of = jax.random.split(jax.random.key(seed), 21)
    part_splits = jax.random.split(jax.random.fold_in(key_of[20], part), 21)
    volume = centred(part_splits[0], (C, Z, Y, X), 1.0, 6.0, ((2, 64),))
    dual_state = centred(part_splits[1], (C, Z, V, U), 1.0, 6.0, ((2, 64),))
    sinogram = centred(part_splits[2], (NB, Z, V, U), 1.0, 6.0, ((2, 64),))
    cot_volume = centred(part_splits[3], (C, Z, Y, X), 1.0, 6.0, ((2, 64),))
    cot_dual = centred(part_splits[4], (C, Z, V, U), 1.0, 6.0, ((2, 64),))
    basis_table = centred(key_of[5], (NE, C), C ** -0.5, 1.0)
    bin_energy = with_ends(jax.random.randint(key_of[6], (NB,), 0, NE), jax.random.fold_in(key_of[6], 1), 0, NE - 1).astype(jnp.int32)
    footprint_table = centred(key_of[7], (NOFF, YT * X, VB * UW), (8 * YT * X) ** -0.5, 0.0625)
    hit_tile = draw_hit_tile(jax.random.fold_in(key_of[20], 71), part)
    hit_table = with_ends(jax.random.randint(key_of[9], (BLOCKS, K_MAX), 0, NOFF), jax.random.fold_in(key_of[9], 1), 0, NOFF - 1).astype(jnp.int32)
    hit_column = with_ends(jax.random.randint(key_of[10], (BLOCKS, K_MAX), 0, U // UW), jax.random.fold_in(key_of[10], 1), 0, (U // UW) - 1).astype(jnp.int32)
    hit_count = draw_hit_count(jax.random.fold_in(key_of[20], 71), part)
    primal_inner = centred(key_of[12], (27, C, C + NB), (27 * (C + NB)) ** -0.5, 0.1875)
    primal_inner_bias = centred(key_of[13], (C,), 0.5, 3.0, (), jnp.float32)
    primal_outer = centred(key_of[14], (27, C, C), (27 * C) ** -0.5, 0.21875)
    primal_outer_bias = centred(key_of[15], (C,), 0.5, 3.0, (), jnp.float32)
    dual_inner = centred(key_of[16], (27, C, C + 2 * NB), (27 * (C + 2 * NB)) ** -0.5, 0.1875)
    dual_inner_bias = centred(key_of[17], (C,), 0.5, 3.0, (), jnp.float32)
    dual_outer = centred(key_of[18], (27, C, C), (27 * C) ** -0.5, 0.21875)
    dual_outer_bias = centred(key_of[19], (C,), 0.5, 3.0, (), jnp.float32)
    return dict(volume=volume, dual_state=dual_state, sinogram=sinogram, cot_volume=cot_volume, cot_dual=cot_dual, basis_table=basis_table, bin_energy=bin_energy, footprint_table=footprint_table, hit_tile=hit_tile, hit_table=hit_table, hit_column=hit_column, hit_count=hit_count, primal_inner=primal_inner, primal_inner_bias=primal_inner_bias, primal_outer=primal_outer, primal_outer_bias=primal_outer_bias, dual_inner=dual_inner, dual_inner_bias=dual_inner_bias, dual_outer=dual_outer, dual_outer_bias=dual_outer_bias)


precise = lax.Precision.HIGHEST

def hit_pairs(hit_tile, hit_table, hit_column, hit_count, tables, columns):
    blocks = hit_tile.shape[0]
    entries = hit_tile.shape[1]
    live_mask = (jnp.arange(entries)[None, :] < hit_count[:, None]).astype(jnp.float32)
    tile_onehot = (hit_tile[:, :, None] == jnp.arange(blocks)[None, None, :]).astype(jnp.float32)
    table_onehot = (hit_table[:, :, None] == jnp.arange(tables)[None, None, :]).astype(jnp.float32)
    column_onehot = (hit_column[:, :, None] == jnp.arange(columns)[None, None, :]).astype(jnp.float32)
    return jnp.einsum('bk,bkt,bko,bkc->btoc', live_mask, tile_onehot, table_onehot, column_onehot, precision=precise)

def silu_slope(pre_values):
    sigmoid = jax.nn.sigmoid(pre_values)
    return sigmoid * (1.0 + pre_values * (1.0 - sigmoid))

def volume_pad(source):
    return jnp.pad(source, ((0, 0), (1, 1), (1, 1), (1, 1)))

def cycle_pad(source):
    wrapped = jnp.concatenate([source[:, :, -1:], source, source[:, :, :1]], axis=2)
    return jnp.pad(wrapped, ((0, 0), (1, 1), (0, 0), (1, 1)))

def conv_apply(padded, weight, bias_vector):
    slices = padded.shape[1] - 2
    height = padded.shape[2] - 2
    breadth = padded.shape[3] - 2
    padded_wide = padded.astype(jnp.float32)
    weight_wide = weight.astype(jnp.float32)
    running = jnp.zeros((weight.shape[1], slices, height, breadth), jnp.float32)
    for tap_index in range(27):
        shift_z, shift_y, shift_x = (tap_index // 9, tap_index // 3 % 3, tap_index % 3)
        window = padded_wide[:, shift_z:shift_z + slices, shift_y:shift_y + height, shift_x:shift_x + breadth]
        running = running + jnp.einsum('oc,czyx->ozyx', weight_wide[tap_index], window, precision=precise)
    return running + bias_vector[:, None, None, None]

def conv_adjoint(padded, weight):
    slices = padded.shape[1] - 2
    height = padded.shape[2] - 2
    breadth = padded.shape[3] - 2
    padded_wide = padded.astype(jnp.float32)
    weight_wide = weight.astype(jnp.float32)
    running = jnp.zeros((weight.shape[2], slices, height, breadth), jnp.float32)
    for tap_index in range(27):
        shift_z, shift_y, shift_x = (tap_index // 9, tap_index // 3 % 3, tap_index % 3)
        window = padded_wide[:, 2 - shift_z:2 - shift_z + slices, 2 - shift_y:2 - shift_y + height, 2 - shift_x:2 - shift_x + breadth]
        running = running + jnp.einsum('oc,ozyx->czyx', weight_wide[tap_index], window, precision=precise)
    return running

def weight_grad(cotangent, padded):
    slices = cotangent.shape[1]
    height = cotangent.shape[2]
    breadth = cotangent.shape[3]
    padded_wide = padded.astype(jnp.float32)
    cot_wide = cotangent.astype(jnp.float32)
    per_tap = []
    for tap_index in range(27):
        shift_z, shift_y, shift_x = (tap_index // 9, tap_index // 3 % 3, tap_index % 3)
        window = padded_wide[:, shift_z:shift_z + slices, shift_y:shift_y + height, shift_x:shift_x + breadth]
        per_tap.append(jnp.einsum('ozyx,czyx->oc', cot_wide, window, precision=precise))
    return jnp.stack(per_tap)

def project(bin_images, footprint_table, pairs):
    bin_count, slices, ycells, xcells = bin_images.shape
    blocks = pairs.shape[0]
    columns = pairs.shape[3]
    row_count = ycells // blocks
    height = bin_count * slices
    tile_rows = bin_images.reshape(bin_count, slices, blocks, row_count, xcells).transpose(2, 0, 1, 3, 4)
    tile_rows = tile_rows.reshape(blocks, height, row_count * xcells).astype(jnp.float32)
    table_wide = footprint_table.astype(jnp.float32)
    footprints = jnp.einsum('tqs,osw->toqw', tile_rows, table_wide, precision=precise)
    windows = jnp.einsum('btoc,toqw->bcqw', pairs, footprints, precision=precise)
    view_count = footprint_table.shape[2] // UW
    layout = windows.reshape(blocks, columns, bin_count, slices, view_count, UW).transpose(2, 3, 0, 4, 1, 5)
    return layout.reshape(bin_count, slices, blocks * view_count, columns * UW)

def backproject(signal, footprint_table, pairs):
    bin_count, slices, all_views, detector = signal.shape
    blocks = pairs.shape[0]
    view_count = all_views // blocks
    columns = detector // UW
    height = bin_count * slices
    windows = signal.reshape(bin_count, slices, blocks, view_count, columns, UW).transpose(2, 4, 0, 1, 3, 5)
    windows = windows.reshape(blocks, columns, height, view_count * UW).astype(jnp.float32)
    grouped = jnp.einsum('btoc,bcqw->toqw', pairs, windows, precision=precise)
    tile_sums = jnp.einsum('toqw,osw->tqs', grouped, footprint_table.astype(jnp.float32), precision=precise)
    cell_count = tile_sums.shape[2] // YT
    layout = tile_sums.reshape(blocks, bin_count, slices, YT, cell_count).transpose(1, 2, 0, 3, 4)
    return layout.reshape(bin_count, slices, blocks * YT, cell_count)

def reference(volume, dual_state, sinogram, cot_volume, cot_dual, basis_table, bin_energy, footprint_table, hit_tile, hit_table, hit_column, hit_count, primal_inner, primal_inner_bias, primal_outer, primal_outer_bias, dual_inner, dual_inner_bias, dual_outer, dual_outer_bias):
    channels = volume.shape[0]
    bin_count = sinogram.shape[0]
    columns = dual_state.shape[3] // UW
    pairs = hit_pairs(hit_tile, hit_table, hit_column, hit_count, footprint_table.shape[0], columns)
    energy_onehot = (bin_energy[:, None] == jnp.arange(basis_table.shape[0])[None, :]).astype(jnp.float32)
    mixing = jnp.dot(energy_onehot, basis_table.astype(jnp.float32), precision=precise).astype(jnp.bfloat16)
    mixing_wide = mixing.astype(jnp.float32)
    bin_images = jnp.einsum('nc,czyx->nzyx', mixing_wide, volume.astype(jnp.float32), precision=precise).astype(jnp.bfloat16)
    projected = project(bin_images, footprint_table, pairs).astype(jnp.bfloat16)
    dual_in = jnp.concatenate([dual_state, projected, sinogram], axis=0)
    dual_in_pad = cycle_pad(dual_in)
    dual_pre = conv_apply(dual_in_pad, dual_inner, dual_inner_bias)
    dual_hidden = jax.nn.silu(dual_pre).astype(jnp.bfloat16)
    dual_hidden_pad = cycle_pad(dual_hidden)
    dual_update = conv_apply(dual_hidden_pad, dual_outer, dual_outer_bias)
    new_dual = (dual_state.astype(jnp.float32) + dual_update).astype(jnp.bfloat16)
    backprojected = backproject(new_dual[:bin_count], footprint_table, pairs).astype(jnp.bfloat16)
    primal_in = jnp.concatenate([volume, backprojected], axis=0)
    primal_in_pad = volume_pad(primal_in)
    primal_pre = conv_apply(primal_in_pad, primal_inner, primal_inner_bias)
    primal_hidden = jax.nn.silu(primal_pre).astype(jnp.bfloat16)
    primal_hidden_pad = volume_pad(primal_hidden)
    primal_update = conv_apply(primal_hidden_pad, primal_outer, primal_outer_bias)
    new_volume = (volume.astype(jnp.float32) + primal_update).astype(jnp.bfloat16)
    hidden_grad = conv_adjoint(volume_pad(cot_volume), primal_outer)
    pre_grad = (hidden_grad * silu_slope(primal_pre)).astype(jnp.bfloat16)
    in_grad = conv_adjoint(volume_pad(pre_grad), primal_inner)
    back_grad = in_grad[channels:].astype(jnp.bfloat16)
    toward_dual = project(back_grad, footprint_table, pairs)
    dual_total = jnp.concatenate([cot_dual[:bin_count].astype(jnp.float32) + toward_dual, cot_dual[bin_count:].astype(jnp.float32)], axis=0)
    dual_cot = dual_total.astype(jnp.bfloat16)
    dual_hidden_grad = conv_adjoint(cycle_pad(dual_cot), dual_outer)
    dual_pre_grad = (dual_hidden_grad * silu_slope(dual_pre)).astype(jnp.bfloat16)
    dual_in_grad = conv_adjoint(cycle_pad(dual_pre_grad), dual_inner)
    dual_grad = (dual_total + dual_in_grad[:channels]).astype(jnp.bfloat16)
    projected_grad = dual_in_grad[channels:channels + bin_count].astype(jnp.bfloat16)
    bins_grad = backproject(projected_grad, footprint_table, pairs)
    volume_grad = (cot_volume.astype(jnp.float32) + in_grad[:channels] + jnp.einsum('nc,nzyx->czyx', mixing_wide, bins_grad, precision=precise)).astype(jnp.bfloat16)
    primal_inner_grad = weight_grad(pre_grad, primal_in_pad)
    primal_outer_grad = weight_grad(cot_volume, primal_hidden_pad)
    dual_inner_grad = weight_grad(dual_pre_grad, dual_in_pad)
    dual_outer_grad = weight_grad(dual_cot, dual_hidden_pad)
    return (new_volume, new_dual, volume_grad, dual_grad, primal_inner_grad, primal_outer_grad, dual_inner_grad, dual_outer_grad)
```

```python
import functools

import jax
import jax.numpy as jnp
from jax import lax
from jax.experimental import pallas as pl
from jax.experimental.pallas import tpu as pltpu
from jax.sharding import PartitionSpec as P

F32 = jnp.float32
BF16 = jnp.bfloat16
MESH = pl.DeviceIdType.MESH
AXIS = "view"
UW = 128
LANES = 128
OFFS = (-2, -1, 1, 2)


def dot(a, b):
    return jnp.dot(a, b, preferred_element_type=F32)


def dot_nt(a, b):
    return lax.dot_general(a, b, (((1,), (1,)), ((), ())), preferred_element_type=F32)


def sigmoid(a):
    return 1.0 / (1.0 + jnp.exp(-a))


def padded(piece, width):
    if piece.shape[1] == width:
        return piece
    return jnp.concatenate(
        [piece, jnp.zeros((piece.shape[0], width - piece.shape[1]), piece.dtype)], axis=1
    )


def forward_weights(weight, target, width):
    outs = weight.shape[1]
    for zo in range(2):
        pieces = []
        for j in range(3):
            for zi in range(2):
                for l in range(3):
                    tap = 9 * (zi - zo + 1) + 3 * j + l
                    pieces.append(padded(weight[tap].astype(F32), width))
        target[zo * outs : (zo + 1) * outs, :] = jnp.concatenate(pieces, axis=1).astype(BF16)


def adjoint_weights(weight, target, width):
    rows = []
    for j in range(3):
        for zi in range(2):
            for l in range(3):
                pair = []
                for zo in range(2):
                    tap = 26 - (9 * (zi - zo + 1) + 3 * j + l)
                    pair.append(padded(weight[tap].astype(F32), width))
                rows.append(padded(jnp.concatenate(pair, axis=1), LANES))
    tall = jnp.concatenate(rows, axis=0)
    target[...] = tall.T[: 2 * width].astype(BF16)


def shifted(block):
    wide = block.astype(F32)
    last = block.shape[1] - 1
    lane = lax.broadcasted_iota(jnp.int32, wide.shape, 1)
    low = jnp.where(lane == 0, 0.0, pltpu.roll(wide, 1, 1)).astype(BF16)
    high = jnp.where(lane == last, 0.0, pltpu.roll(wide, last, 1)).astype(BF16)
    return low, high


def fill(rows, y, z, first, block):
    height = block.shape[0]
    low, high = shifted(block)
    rows[y, z, 0, first : first + height, :] = low
    rows[y, z, 1, first : first + height, :] = block
    rows[y, z, 2, first : first + height, :] = high


def taken(rows, y):
    part = rows[pl.ds(y, 3)]
    return part.reshape(part.shape[0] * part.shape[1] * part.shape[2] * part.shape[3], part.shape[4])


def weight_sum(rows, first, cots):
    total = None
    for r, cot in enumerate(cots):
        high, low = cot[32:64], cot[0:32]
        none = jnp.zeros_like(low)
        for zi in range(2):
            spread = [high, low, none, none] if zi == 0 else [none, high, low, none]
            part = rows[first + r : first + r + 3, zi]
            part = part.reshape(part.shape[0] * part.shape[1] * part.shape[2], part.shape[3])
            term = dot_nt(part, jnp.concatenate(spread, axis=0))
            total = term if total is None else total + term
    return total


def kernel(
    n,
    tw,
    pc,
    vol,
    cvol,
    ds,
    cd,
    sino,
    mix,
    mix_t,
    table,
    wpi,
    wpo,
    wdi,
    wdo,
    bpi,
    bpo,
    bdi,
    bdo,
    nv,
    nd,
    vg,
    dg,
    gp,
    gd,
    fpi,
    fpo,
    fdi,
    fdo,
    api,
    apo,
    adi,
    ado,
    s_d,
    s_dh,
    s_p,
    s_ph,
    s_c,
    s_pg,
    s_dc,
    s_dpg,
    ds_h,
    si_h,
    pr_h,
    vol_h,
    cvol_h,
    cd_h,
    bp_h,
    dc_h,
    pr_own,
    bp_own,
    dc_own,
    dpre,
    ppre,
    hgrad,
    ingrad,
    dtotal,
    dhg,
    rsum,
    pack,
    outbox,
    inbox,
    rs_out,
    rs_in,
    ag_own,
    ag_in,
    send,
    recv,
    hsend,
    hrecv,
):
    me = lax.axis_index(AXIS)
    channels = ds.shape[0] // 2
    width = ds.shape[1]
    columns = width // UW
    tables = table.shape[0]
    chunk = ag_own.shape[1]

    def to(offset):
        return lax.rem(me + offset + n, n)

    barrier = pltpu.get_barrier_semaphore()

    @pl.loop(1, n)
    def _(k):
        pl.semaphore_signal(
            barrier, inc=1, device_id={AXIS: lax.rem(me + k, n)}, device_id_type=MESH
        )

    def exchange(source, target, phase, same):
        @pl.loop(0, n - 1)
        def _(k):
            half = k // 2
            ahead = jnp.where(k % 2 == 0, n // 2 + half, n // 2 - half - 1)
            peer = lax.rem(me + ahead, n)
            pltpu.make_async_remote_copy(
                src_ref=source if same else source.at[peer],
                dst_ref=target.at[me],
                send_sem=send.at[phase],
                recv_sem=recv.at[phase],
                device_id={AXIS: peer},
                device_id_type=MESH,
            ).start()

        target[me] = source[...] if same else source[me]

    def all_of(target, phase):
        return pltpu.make_async_remote_copy(
            src_ref=target.at[pl.ds(0, n - 1)],
            dst_ref=target.at[pl.ds(0, n - 1)],
            send_sem=send.at[phase],
            recv_sem=recv.at[phase],
            device_id={AXIS: to(1)},
            device_id_type=MESH,
        )

    halos = []

    def halo(source, target, offsets, base):
        copies = []
        for slot, offset in enumerate(offsets):
            there = len(offsets) - 1 - slot
            copies.append(
                pltpu.make_async_remote_copy(
                    src_ref=source,
                    dst_ref=target.at[there],
                    send_sem=hsend.at[base + there],
                    recv_sem=hrecv.at[base + there],
                    device_id={AXIS: to(offset)},
                    device_id_type=MESH,
                )
            )
        for copy in copies:
            copy.start()
        halos.extend(copies)
        return copies

    def footprints(q):
        return [dot(q, table[o]) for o in range(tables)]

    def spread(values, scale, target):
        count = len(values)

        @pl.loop(0, n)
        def _(b):
            total = scale[b * count] * values[0]
            for o in range(1, count):
                total = total + scale[b * count + o] * values[o]
            target[b] = total.astype(BF16)

    def gathered(source, scale, count):
        def step(t, totals):
            block = source[t].astype(F32)
            return tuple(totals[c] + scale[t * count + c] * block for c in range(count))

        start = tuple(jnp.zeros(source.shape[1:], F32) for _ in range(count))
        return lax.fori_loop(0, n, step, start, unroll=4)

    def q_of(y0, y1):
        return jnp.concatenate([y0, y1], axis=1)

    def tile_sums(groups):
        total = None
        for o in range(tables):
            high = groups[o].astype(BF16)
            low = (groups[o] - high.astype(F32)).astype(BF16)
            term = dot_nt(jnp.concatenate([high, low], axis=0), table[o])
            total = term if total is None else total + term
        return total[0:8] + total[8:16]

    bins = q_of(dot(mix[...], vol[0]), dot(mix[...], vol[1])).astype(BF16)
    spread(footprints(bins), tw, outbox.at[0])
    forward_weights(wdi, fdi, 48)
    forward_weights(wdo, fdo, 32)
    forward_weights(wpi, fpi, 48)
    forward_weights(wpo, fpo, 32)
    adjoint_weights(wpo, apo, 32)
    adjoint_weights(wpi, api, 48)
    adjoint_weights(wdo, ado, 32)
    adjoint_weights(wdi, adi, 48)
    pl.semaphore_wait(barrier, n - 1)
    exchange(outbox.at[0], inbox.at[0], 0, False)
    ds_copies = halo(ds, ds_h, OFFS, 0)
    si_copies = halo(sino, si_h, OFFS, 4)

    def fill_views(rows, own, others, first):
        for z in range(2):
            fill(rows, 2, z, first, own[z * channels : (z + 1) * channels, :])
        for slot, view in enumerate((0, 1, 3, 4)):
            for z in range(2):
                fill(rows, view, z, first, others[slot, z * channels : (z + 1) * channels, :])

    for copy in ds_copies:
        copy.wait_recv()
    fill_views(s_d, ds, ds_h, 0)
    for copy in si_copies:
        copy.wait_recv()

    all_of(inbox.at[0], 0).wait_recv()
    windows = gathered(inbox.at[0], pc, columns)
    pr_own[...] = jnp.concatenate(windows, axis=1).astype(BF16)
    pr_copies = halo(pr_own, pr_h, OFFS, 8)
    vol_copies = halo(vol, vol_h, (-1, 1), 12)
    cvol_copies = halo(cvol, cvol_h, (-1, 1), 14)

    def fill_tail(view, projected, measured):
        for z in range(2):
            block = jnp.concatenate(
                [
                    projected[z * 4 : z * 4 + 4].astype(F32),
                    measured[z * 4 : z * 4 + 4].astype(F32),
                    jnp.zeros((8, width), F32),
                ],
                axis=0,
            ).astype(BF16)
            fill(s_d, view, z, channels, block)

    fill_tail(2, pr_own[...], sino[...])
    for copy in pr_copies:
        copy.wait_recv()
    for slot, view in enumerate((0, 1, 3, 4)):
        fill_tail(view, pr_h[slot], si_h[slot])

    @pl.loop(0, 3)
    def _(v):
        pre = dot(fdi[...], taken(s_d, v)) + bdi[...]
        dpre[v] = pre
        hidden = (pre * sigmoid(pre)).astype(BF16)
        for z in range(2):
            fill(s_dh, v, z, 0, hidden[z * channels : (z + 1) * channels])

    update = dot(fdo[...], taken(s_dh, 0)) + bdo[...]
    fresh = (ds[...].astype(F32) + update).astype(BF16)
    nd[...] = fresh

    def bins_of(block, stride, first):
        return jnp.concatenate(
            [block[first : first + 4], block[stride + first : stride + first + 4]], axis=0
        )

    def parts_of(signal):
        return [signal[:, c * UW : (c + 1) * UW] for c in range(columns)]

    spread(parts_of(bins_of(fresh.astype(F32), channels, 0)), pc, outbox.at[1])
    exchange(outbox.at[1], inbox.at[1], 1, False)
    cd_copies = halo(cd, cd_h, OFFS, 16)

    low_in = jnp.where(me > 0, 1.0, 0.0).astype(F32)
    high_in = jnp.where(me < n - 1, 1.0, 0.0).astype(F32)

    def fill_rows(rows, own, others):
        for y in range(2):
            for z in range(2):
                part = slice(z * channels, (z + 1) * channels)
                fill(rows, 2 + y, z, 0, own[y, part, :])
                fill(rows, y, z, 0, (others[0, y, part, :].astype(F32) * low_in).astype(BF16))
                fill(rows, 4 + y, z, 0, (others[1, y, part, :].astype(F32) * high_in).astype(BF16))

    for copy in cvol_copies:
        copy.wait_recv()
    fill_rows(s_c, cvol, cvol_h)

    @pl.loop(0, 4)
    def _(r):
        hgrad[r] = dot(apo[...], taken(s_c, r))

    for copy in vol_copies:
        copy.wait_recv()
    fill_rows(s_p, vol, vol_h)

    all_of(inbox.at[1], 1).wait_recv()
    summed = tile_sums(gathered(inbox.at[1], tw, tables))
    bp_own[...] = summed.astype(BF16)
    bp_copies = halo(bp_own, bp_h, (-1, 1), 20)

    def fill_back(row, block):
        for z in range(2):
            part = jnp.concatenate(
                [block[z * 4 : z * 4 + 4], jnp.zeros((12, width), F32)], axis=0
            ).astype(BF16)
            fill(s_p, row, z, channels, part)

    own_back = bp_own[...].astype(F32)
    for y in range(2):
        fill_back(2 + y, own_back[:, y * width : (y + 1) * width])
    for copy in bp_copies:
        copy.wait_recv()
    low_back = bp_h[0].astype(F32) * low_in
    high_back = bp_h[1].astype(F32) * high_in
    for y in range(2):
        fill_back(y, low_back[:, y * width : (y + 1) * width])
        fill_back(4 + y, high_back[:, y * width : (y + 1) * width])

    @pl.loop(0, 4)
    def _(r):
        pre = dot(fpi[...], taken(s_p, r)) + bpi[...]
        ppre[r] = pre
        inside = jnp.where(r == 0, low_in, jnp.where(r == 3, high_in, 1.0))
        s = sigmoid(pre)
        grad = (hgrad[r] * (s * (1.0 + pre * (1.0 - s))) * inside).astype(BF16)
        for z in range(2):
            fill(s_pg, r, z, 0, grad[z * channels : (z + 1) * channels])

    for r in range(2):
        ingrad[r] = dot(api[...], taken(s_pg, r))
    back = q_of(bins_of(ingrad[0], 48, channels), bins_of(ingrad[1], 48, channels)).astype(BF16)
    spread(footprints(back), tw, outbox.at[2])
    exchange(outbox.at[2], inbox.at[2], 2, False)

    @pl.loop(0, 4)
    def _(r):
        pre = ppre[r]
        inside = jnp.where(r == 0, low_in, jnp.where(r == 3, high_in, 1.0))
        hidden = (pre * sigmoid(pre) * inside).astype(BF16)
        for z in range(2):
            fill(s_ph, r, z, 0, hidden[z * channels : (z + 1) * channels])

    def packed(inner, outer, side):
        for k in range(9):
            rsum[k * 40 : (k + 1) * 40, :] = inner[k * 48 : k * 48 + 40]
        rsum[360:648, :] = outer
        lane = lax.broadcasted_iota(jnp.int32, (160, LANES), 1)
        tail = rsum[488:648, :]
        for i in range(3):
            moved = tail if i == 3 else pltpu.roll(tail, 96 - 32 * i, 1)
            pack[i * 160 : (i + 1) * 160, :] = jnp.where(
                lane < 96, rsum[i * 160 : (i + 1) * 160, :], moved
            )
        pack[480:488, :] = rsum[480:488, :]
        pack[488:512, :] = jnp.zeros((24, LANES), F32)
        rs_out[side] = pack[...].reshape(n, chunk, LANES).astype(BF16)

    def own_rows(rows, y):
        return jnp.concatenate([rows[y, 0, 1], rows[y, 1, 1]], axis=0)

    packed(
        weight_sum(s_p, 1, [own_rows(s_pg, 1), own_rows(s_pg, 2)]),
        weight_sum(s_ph, 0, [cvol[0], cvol[1]]),
        0,
    )
    exchange(rs_out.at[0], rs_in.at[0], 4, False)

    for r in range(2):
        change = dot(fpo[...], taken(s_ph, r)) + bpo[...]
        nv[r] = (vol[r].astype(F32) + change).astype(BF16)

    for copy in cd_copies:
        copy.wait_recv()

    all_of(inbox.at[2], 2).wait_recv()
    toward = jnp.concatenate(gathered(inbox.at[2], pc, columns), axis=1)
    own_cot = cd[...].astype(F32)
    dtotal[...] = own_cot
    dtotal[0:4, :] = own_cot[0:4] + toward[0:4]
    dtotal[channels : channels + 4, :] = own_cot[channels : channels + 4] + toward[4:8]
    dc_own[...] = bins_of(dtotal[...], channels, 0).astype(BF16)
    dc_copies = halo(dc_own, dc_h, OFFS, 22)
    own_total = dtotal[...].astype(BF16)
    for z in range(2):
        fill(s_dc, 2, z, 0, own_total[z * channels : (z + 1) * channels])
    for copy in dc_copies:
        copy.wait_recv()
    for slot, view in enumerate((0, 1, 3, 4)):
        for z in range(2):
            block = jnp.concatenate(
                [
                    dc_h[slot, z * 4 : z * 4 + 4, :].astype(F32),
                    cd_h[slot, z * channels + 4 : (z + 1) * channels, :].astype(F32),
                ],
                axis=0,
            ).astype(BF16)
            fill(s_dc, view, z, 0, block)

    @pl.loop(0, 3)
    def _(v):
        pre = dpre[v]
        s = sigmoid(pre)
        grad = (dot(ado[...], taken(s_dc, v)) * (s * (1.0 + pre * (1.0 - s)))).astype(BF16)
        for z in range(2):
            fill(s_dpg, v, z, 0, grad[z * channels : (z + 1) * channels])

    packed(
        weight_sum(s_d, 1, [own_rows(s_dpg, 1)]),
        weight_sum(s_dh, 0, [own_total]),
        1,
    )
    exchange(rs_out.at[1], rs_in.at[1], 5, False)
    dhg[...] = dot(adi[...], taken(s_dpg, 0))
    spread(parts_of(bins_of(dhg[...], 48, channels).astype(BF16).astype(F32)), pc, outbox.at[3])
    exchange(outbox.at[3], inbox.at[3], 3, False)
    for z in range(2):
        part = slice(z * channels, (z + 1) * channels)
        dg[part, :] = (dtotal[part, :] + dhg[z * 48 : z * 48 + channels, :]).astype(BF16)

    def reduced(side):
        def step(t, total):
            return total + rs_in[side, t].astype(F32)

        total = lax.fori_loop(0, n, step, jnp.zeros((chunk, LANES), F32), unroll=4)
        ag_own[side] = total.astype(BF16)

    all_of(rs_in.at[0], 4).wait_recv()
    reduced(0)
    exchange(ag_own.at[0], ag_in.at[0], 6, True)
    all_of(rs_in.at[1], 5).wait_recv()
    reduced(1)
    exchange(ag_own.at[1], ag_in.at[1], 7, True)

    all_of(inbox.at[3], 3).wait_recv()
    final = tile_sums(gathered(inbox.at[3], tw, tables))
    high = final.astype(BF16)
    low = (final - high.astype(F32)).astype(BF16)
    both = jnp.concatenate([high.astype(F32), low.astype(F32)], axis=0).astype(BF16)
    for y in range(2):
        mixed = dot(mix_t[...], both[:, y * width : (y + 1) * width])
        for z in range(2):
            part = slice(z * channels, (z + 1) * channels)
            vg[y, part, :] = (
                cvol[y, part, :].astype(F32)
                + ingrad[y, z * 48 : z * 48 + channels, :]
                + mixed[part]
            ).astype(BF16)

    all_of(ag_in.at[0], 6).wait_recv()
    gp[...] = ag_in[0].astype(F32).reshape(n * chunk, LANES)
    all_of(ag_in.at[1], 7).wait_recv()
    gd[...] = ag_in[1].astype(F32).reshape(n * chunk, LANES)

    for phase in range(4):
        all_of(inbox.at[phase], phase).wait_send()
    for side in range(2):
        all_of(rs_in.at[side], 4 + side).wait_send()
        all_of(ag_in.at[side], 6 + side).wait_send()
    for copy in halos:
        copy.wait_send()


def unpacked(packed, inner_width, outer_width):
    outs = 32
    main = packed[:488, :96].reshape(488, 3, outs)
    tail = packed[:480, 96:].reshape(3, 160, outs).transpose(1, 0, 2)
    rows = jnp.concatenate([main, tail], axis=0)
    inner = rows[:360].reshape(9, 40, 3, outs)[:, :inner_width]
    outer = rows[360:].reshape(9, 32, 3, outs)
    return (
        inner.transpose(2, 0, 3, 1).reshape(27, outs, inner_width),
        outer.transpose(2, 0, 3, 1).reshape(27, outs, outer_width),
    )


def shards(
    n,
    volume,
    dual_state,
    sinogram,
    cot_volume,
    cot_dual,
    basis_table,
    bin_energy,
    footprint_table,
    hit_tile,
    hit_table,
    hit_column,
    hit_count,
    primal_inner,
    primal_inner_bias,
    primal_outer,
    primal_outer_bias,
    dual_inner,
    dual_inner_bias,
    dual_outer,
    dual_outer_bias,
):
    me = lax.axis_index(AXIS)
    channels, slices, row_count, width = volume.shape
    bin_count = sinogram.shape[0]
    columns = width // UW
    tables = footprint_table.shape[0]
    entries = hit_tile.shape[1]
    both = slices * channels

    live = jnp.arange(entries)[None, :] < hit_count[:, None]
    mine = live & (hit_tile == me)
    toward = jnp.sum(
        (mine[:, None, :] & (hit_table[:, None, :] == jnp.arange(tables)[None, :, None])).astype(F32),
        axis=2,
    ).reshape(-1)
    own_tile = lax.dynamic_index_in_dim(hit_tile, me, 0, keepdims=False)
    own_column = lax.dynamic_index_in_dim(hit_column, me, 0, keepdims=False)
    own_live = jnp.arange(entries) < lax.dynamic_index_in_dim(hit_count, me, 0, keepdims=False)
    placing = jnp.sum(
        (
            (own_live & (own_tile == jnp.arange(n)[:, None]))[:, None, :]
            & (own_column == jnp.arange(columns)[None, :, None])
        ).astype(F32),
        axis=2,
    ).reshape(-1)

    energy = (bin_energy[:, None] == jnp.arange(basis_table.shape[0])[None, :]).astype(BF16)
    mixing = jnp.dot(energy, basis_table, preferred_element_type=F32).astype(BF16)
    mix = jnp.concatenate(
        [
            jnp.concatenate([mixing, jnp.zeros_like(mixing)], axis=1),
            jnp.concatenate([jnp.zeros_like(mixing), mixing], axis=1),
        ],
        axis=0,
    )
    mix_t = jnp.concatenate([mix.T, mix.T], axis=1)

    vol = volume.transpose(2, 1, 0, 3).reshape(row_count, both, width)
    cvol = cot_volume.transpose(2, 1, 0, 3).reshape(row_count, both, width)
    ds = dual_state.transpose(2, 1, 0, 3).reshape(both, width)
    cd = cot_dual.transpose(2, 1, 0, 3).reshape(both, width)
    sino = sinogram.transpose(2, 1, 0, 3).reshape(slices * bin_count, width)
    biases = [
        jnp.concatenate([b, b]).reshape(both, 1)
        for b in (primal_inner_bias, primal_outer_bias, dual_inner_bias, dual_outer_bias)
    ]
    chunk = 512 // n
    vmem = pl.BlockSpec(memory_space=pltpu.VMEM)
    smem = pl.BlockSpec(memory_space=pltpu.SMEM)
    shape = jax.ShapeDtypeStruct

    def rows_of(y, c):
        return pltpu.VMEM((y, 2, 3, c, width), BF16)

    messages = (n, slices * bin_count, UW)
    new_volume, new_dual, volume_grad, dual_grad, packed_primal, packed_dual = pl.pallas_call(
        functools.partial(kernel, n),
        out_shape=(
            shape((row_count, both, width), BF16),
            shape((both, width), BF16),
            shape((row_count, both, width), BF16),
            shape((both, width), BF16),
            shape((n * chunk, LANES), F32),
            shape((n * chunk, LANES), F32),
        ),
        in_specs=[smem, smem] + [vmem] * 16,
        out_specs=(vmem,) * 6,
        scratch_shapes=[
            pltpu.VMEM((64, 18 * 48), BF16),
            pltpu.VMEM((64, 18 * 32), BF16),
            pltpu.VMEM((64, 18 * 48), BF16),
            pltpu.VMEM((64, 18 * 32), BF16),
            pltpu.VMEM((96, 18 * 32), BF16),
            pltpu.VMEM((64, 18 * 32), BF16),
            pltpu.VMEM((96, 18 * 32), BF16),
            pltpu.VMEM((64, 18 * 32), BF16),
            rows_of(5, 48),
            rows_of(3, 32),
            rows_of(6, 48),
            rows_of(4, 32),
            rows_of(6, 32),
            rows_of(4, 32),
            rows_of(5, 32),
            rows_of(3, 32),
            pltpu.VMEM((4, both, width), BF16),
            pltpu.VMEM((4, 8, width), BF16),
            pltpu.VMEM((4, 8, width), BF16),
            pltpu.VMEM((2, row_count, both, width), BF16),
            pltpu.VMEM((2, row_count, both, width), BF16),
            pltpu.VMEM((4, both, width), BF16),
            pltpu.VMEM((2, 8, row_count * width), BF16),
            pltpu.VMEM((4, 8, width), BF16),
            pltpu.VMEM((8, width), BF16),
            pltpu.VMEM((8, row_count * width), BF16),
            pltpu.VMEM((8, width), BF16),
            pltpu.VMEM((3, both, width), F32),
            pltpu.VMEM((4, both, width), F32),
            pltpu.VMEM((4, both, width), F32),
            pltpu.VMEM((2, 96, width), F32),
            pltpu.VMEM((both, width), F32),
            pltpu.VMEM((96, width), F32),
            pltpu.VMEM((648, LANES), F32),
            pltpu.VMEM((512, LANES), F32),
            pltpu.VMEM((4,) + messages, BF16),
            pltpu.VMEM((4,) + messages, BF16),
            pltpu.VMEM((2, n, chunk, LANES), BF16),
            pltpu.VMEM((2, n, chunk, LANES), BF16),
            pltpu.VMEM((2, chunk, LANES), BF16),
            pltpu.VMEM((2, n, chunk, LANES), BF16),
            pltpu.SemaphoreType.DMA((8,)),
            pltpu.SemaphoreType.DMA((8,)),
            pltpu.SemaphoreType.DMA((26,)),
            pltpu.SemaphoreType.DMA((26,)),
        ],
        compiler_params=pltpu.CompilerParams(
            collective_id=0, has_side_effects=True, vmem_limit_bytes=60 * 1024 * 1024
        ),
    )(
        toward,
        placing,
        vol,
        cvol,
        ds,
        cd,
        sino,
        mix,
        mix_t,
        footprint_table,
        primal_inner,
        primal_outer,
        dual_inner,
        dual_outer,
        *biases,
    )

    def volume_of(block):
        return block.reshape(row_count, slices, channels, width).transpose(2, 1, 0, 3)

    def view_of(block):
        return block.reshape(1, slices, channels, width).transpose(2, 1, 0, 3)

    return (
        volume_of(new_volume),
        view_of(new_dual),
        volume_of(volume_grad),
        view_of(dual_grad),
        *unpacked(packed_primal, primal_inner.shape[2], channels),
        *unpacked(packed_dual, dual_inner.shape[2], channels),
    )


def solution(mesh):
    part = P(None, "parts", AXIS, None)
    return jax.shard_map(
        functools.partial(shards, mesh.shape[AXIS]),
        mesh=mesh,
        in_specs=(part,) * 5 + (P(),) * 15,
        out_specs=(part,) * 4 + (P("parts", None, None),) * 4,
        check_vma=False,
    )
```

```python
import functools

import jax
import jax.numpy as jnp
from jax import lax
from jax.experimental import pallas as pl
from jax.experimental.pallas import tpu as pltpu
from jax.sharding import PartitionSpec as P

F32 = jnp.float32
BF16 = jnp.bfloat16
MESH = pl.DeviceIdType.MESH
AXIS = "view"
UW = 128
LANES = 128
OFFS = (-2, -1, 1, 2)


def dot(a, b):
    return jnp.dot(a, b, preferred_element_type=F32)


def dot_tn(a, b):
    return lax.dot_general(a, b, (((0,), (0,)), ((), ())), preferred_element_type=F32)


def dot_nt(a, b):
    return lax.dot_general(a, b, (((1,), (1,)), ((), ())), preferred_element_type=F32)


def sigmoid(a):
    return 1.0 / (1.0 + jnp.exp(-a))


def padded(piece, width):
    if piece.shape[1] == width:
        return piece
    return jnp.concatenate(
        [piece, jnp.zeros((piece.shape[0], width - piece.shape[1]), piece.dtype)], axis=1
    )


def forward_weights(weight, target, width):
    outs = weight.shape[1]
    for zo in range(2):
        pieces = []
        for j in range(3):
            for zi in range(2):
                for l in range(3):
                    tap = 9 * (zi - zo + 1) + 3 * j + l
                    pieces.append(padded(weight[tap].astype(F32), width))
        target[zo * outs : (zo + 1) * outs, :] = jnp.concatenate(pieces, axis=1).astype(BF16)


def adjoint_weights(weight, target, width):
    rows = []
    for j in range(3):
        for zi in range(2):
            for l in range(3):
                pair = []
                for zo in range(2):
                    tap = 26 - (9 * (zi - zo + 1) + 3 * j + l)
                    pair.append(padded(weight[tap].astype(F32), width))
                rows.append(padded(jnp.concatenate(pair, axis=1), LANES))
    tall = jnp.concatenate(rows, axis=0)
    target[...] = tall.T[: 2 * width].astype(BF16)


def shifted(block):
    wide = block.astype(F32)
    last = block.shape[1] - 1
    lane = lax.broadcasted_iota(jnp.int32, wide.shape, 1)
    low = jnp.where(lane == 0, 0.0, pltpu.roll(wide, 1, 1)).astype(BF16)
    high = jnp.where(lane == last, 0.0, pltpu.roll(wide, last, 1)).astype(BF16)
    return low, high


def fill(rows, y, z, first, block):
    height = block.shape[0]
    low, high = shifted(block)
    rows[y, z, 0, first : first + height, :] = low
    rows[y, z, 1, first : first + height, :] = block
    rows[y, z, 2, first : first + height, :] = high


def taken(rows, y):
    part = rows[pl.ds(y, 3)]
    return part.reshape(part.shape[0] * part.shape[1] * part.shape[2] * part.shape[3], part.shape[4])


def parted(wide, first, count):
    blocks = [wide[k, pl.ds(first, count, stride=2), :] for k in range(wide.shape[0])]
    return jnp.concatenate(blocks, axis=1).astype(BF16)


def merged(wide, first, block):
    for k in range(wide.shape[0]):
        wide[k, pl.ds(first, block.shape[0], stride=2), :] = block[
            :, k * LANES : (k + 1) * LANES
        ].astype(F32)


def rows_from(wide):
    return jnp.concatenate([wide[k] for k in range(wide.shape[0])], axis=1)


def weight_sum(rows, first, cots):
    total = None
    for r, cot in enumerate(cots):
        high, low = cot[32:64], cot[0:32]
        none = jnp.zeros_like(low)
        for zi in range(2):
            spread = [high, low, none, none] if zi == 0 else [none, high, low, none]
            part = rows[first + r : first + r + 3, zi]
            part = part.reshape(part.shape[0] * part.shape[1] * part.shape[2], part.shape[3])
            term = dot_nt(part, jnp.concatenate(spread, axis=0))
            total = term if total is None else total + term
    return total


def kernel(
    n,
    energy,
    volume,
    dual_state,
    sinogram,
    cot_volume,
    cot_dual,
    basis,
    footprint_table,
    tiles,
    kinds,
    places,
    counts,
    wpi,
    wpo,
    wdi,
    wdo,
    bpi,
    bpo,
    bdi,
    bdo,
    nv,
    nd,
    vg,
    dg,
    gp,
    gd,
    raw_vol,
    raw_cvol,
    raw_ds,
    raw_cd,
    raw_sino,
    table,
    wide,
    vol,
    cvol,
    ds,
    cd,
    sino,
    tw,
    pc,
    fpi,
    fpo,
    fdi,
    fdo,
    api,
    apo,
    adi,
    ado,
    s_d,
    s_dh,
    s_p,
    s_ph,
    s_c,
    s_pg,
    s_dc,
    s_dpg,
    ds_h,
    si_h,
    pr_h,
    vol_h,
    cvol_h,
    cd_h,
    bp_h,
    dc_h,
    pr_own,
    bp_own,
    dc_own,
    dpre,
    ppre,
    hgrad,
    ingrad,
    dtotal,
    dhg,
    rsum,
    pack,
    outbox,
    inbox,
    px_out,
    px_in,
    rs_out,
    rs_in,
    ag_own,
    ag_in,
    load,
    send,
    recv,
    hsend,
    hrecv,
):
    me = lax.axis_index(AXIS)
    chips = n // 2
    chip = me // 2
    core = me % 2
    partner = me + 1 - 2 * core
    channels = ds.shape[0] // 2
    width = ds.shape[1]
    columns = width // UW
    tables = table.shape[0]
    chunk = ag_own.shape[1]

    def to(offset):
        return lax.rem(me + offset + n, n)

    barrier = pltpu.get_barrier_semaphore()

    @pl.loop(1, n)
    def _(k):
        pl.semaphore_signal(
            barrier, inc=1, device_id={AXIS: lax.rem(me + k, n)}, device_id_type=MESH
        )

    loads = [
        pltpu.make_async_copy(source, target, load.at[i])
        for i, (source, target) in enumerate(
            (
                (volume, raw_vol),
                (footprint_table, table),
                (dual_state, raw_ds),
                (sinogram, raw_sino),
                (cot_volume, raw_cvol),
                (cot_dual, raw_cd),
            )
        )
    ]
    for copy in loads:
        copy.start()

    def far_first(k, count):
        half = k // 2
        return jnp.where(k % 2 == 0, count // 2 + half, count // 2 - half - 1)

    def exchange(source, target, phase):
        @pl.loop(0, n - 1)
        def _(k):
            peer = lax.rem(me + far_first(k, n), n)
            pltpu.make_async_remote_copy(
                src_ref=source.at[peer],
                dst_ref=target.at[me],
                send_sem=send.at[phase],
                recv_sem=recv.at[phase],
                device_id={AXIS: peer},
                device_id_type=MESH,
            ).start()

        target[me] = source[me]

    def lanes(source, target, phase, same):
        @pl.loop(0, chips - 1)
        def _(k):
            there = lax.rem(chip + far_first(k, chips), chips)
            pltpu.make_async_remote_copy(
                src_ref=source if same else source.at[there],
                dst_ref=target.at[chip],
                send_sem=send.at[phase],
                recv_sem=recv.at[phase],
                device_id={AXIS: 2 * there + core},
                device_id_type=MESH,
            ).start()

        target[chip] = source[...] if same else source[chip]

    def all_of(target, phase):
        part = target.at[pl.ds(0, target.shape[0] - 1)]
        return pltpu.make_async_remote_copy(
            src_ref=part,
            dst_ref=part,
            send_sem=send.at[phase],
            recv_sem=recv.at[phase],
            device_id={AXIS: to(1)},
            device_id_type=MESH,
        )

    halos = []

    def halo(source, target, offsets, base):
        copies = []
        for slot, offset in enumerate(offsets):
            there = len(offsets) - 1 - slot
            copies.append(
                pltpu.make_async_remote_copy(
                    src_ref=source,
                    dst_ref=target.at[there],
                    send_sem=hsend.at[base + there],
                    recv_sem=hrecv.at[base + there],
                    device_id={AXIS: to(offset)},
                    device_id_type=MESH,
                )
            )
        for copy in copies:
            copy.start()
        halos.extend(copies)
        return copies

    def swap(source, target, phase):
        copy = pltpu.make_async_remote_copy(
            src_ref=source,
            dst_ref=target,
            send_sem=send.at[phase],
            recv_sem=recv.at[phase],
            device_id={AXIS: partner},
            device_id_type=MESH,
        )
        copy.start()
        halos.append(copy)
        return copy

    def footprints(q):
        return [dot(q, table[o]) for o in range(tables)]

    def spread(values, scale, target):
        @pl.loop(0, n, unroll=4)
        def _(b):
            total = scale[0, pl.ds(b, 1), :] * values[0]
            for o in range(1, len(values)):
                total = total + scale[o, pl.ds(b, 1), :] * values[o]
            target[b] = total.astype(BF16)

    def gathered(source, scale, count):
        def step(t, totals):
            block = source[t].astype(F32)
            return tuple(totals[c] + scale[c, pl.ds(t, 1), :] * block for c in range(count))

        start = tuple(jnp.zeros(source.shape[1:], F32) for _ in range(count))
        return lax.fori_loop(0, n, step, start, unroll=4)

    def q_of(y0, y1):
        return jnp.concatenate([y0, y1], axis=1)

    def tile_sums(groups):
        total = None
        for o in range(tables):
            high = groups[o].astype(BF16)
            low = (groups[o] - high.astype(F32)).astype(BF16)
            term = dot_nt(jnp.concatenate([high, low], axis=0), table[o])
            total = term if total is None else total + term
        return total[0:8] + total[8:16]

    entries = tiles.shape[0]
    entry = lax.broadcasted_iota(jnp.int32, (entries, n), 0)
    lane = lax.broadcasted_iota(jnp.int32, (entries, n), 1)
    ones = jnp.ones((entries, LANES), BF16)

    def flags(mask):
        return dot_tn(jnp.where(mask, 1.0, 0.0).astype(BF16), ones)

    tile, kind, place = tiles[...], kinds[...], places[...]
    live = entry < counts[...]
    for o in range(tables):
        tw[o] = flags(live & (tile == me) & (kind == o))

    def own_column(values):
        return jnp.sum(jnp.where(lane == me, values, 0.0), axis=1, keepdims=True)

    own_live = own_column(jnp.where(live, 1.0, 0.0))
    own_tile = own_column(tile.astype(F32))
    own_place = own_column(place.astype(F32))
    hit = (own_tile == lane.astype(F32)) & (own_live > 0.5)
    for c in range(columns):
        pc[c] = flags(hit & (own_place == float(c)))

    row = lax.broadcasted_iota(jnp.int32, (8, 8), 0)
    col = lax.broadcasted_iota(jnp.int32, (8, 8), 1)
    chosen = jnp.zeros((8, 8), F32)
    for b in range(4):
        chosen = chosen + jnp.where((row % 4 == b) & (col == energy[b]), 1.0, 0.0)
    mixing = dot(chosen.astype(BF16), basis[...])
    both_z = jnp.concatenate([mixing, mixing], axis=1)
    row = lax.broadcasted_iota(jnp.int32, both_z.shape, 0)
    col = lax.broadcasted_iota(jnp.int32, both_z.shape, 1)
    mix_wide = jnp.where(row // 4 == col // channels, both_z, 0.0)
    mix = mix_wide.astype(BF16)
    mix_twice = jnp.concatenate([mix_wide, mix_wide], axis=0).astype(BF16)

    def column_of(bias):
        row = lax.broadcasted_iota(jnp.int32, (2 * channels, channels), 0)
        col = lax.broadcasted_iota(jnp.int32, (2 * channels, channels), 1)
        return jnp.sum(jnp.where(row % channels == col, bias[...], 0.0), axis=1, keepdims=True)

    def slab(source, target):
        for z in range(2):
            part = source[:, z].astype(F32).reshape(2 * channels, width)
            for k in range(width // LANES):
                wide[k] = part[:, k * LANES : (k + 1) * LANES]
            for y in range(2):
                target[y, z * channels : (z + 1) * channels, :] = parted(wide, y, channels)

    def view_slab(source, target):
        count = source.shape[0]
        part = source[...].astype(F32).reshape(2 * count, width)
        for k in range(width // LANES):
            wide[k, 0 : 2 * count, :] = part[:, k * LANES : (k + 1) * LANES]
        if count % 16 == 0:
            for z in range(2):
                target[z * count : (z + 1) * count, :] = parted(wide, z, count)
        else:
            target[...] = jnp.concatenate(
                [parted(wide, z, count).astype(F32) for z in range(2)], axis=0
            ).astype(BF16)

    loads[0].wait()
    slab(raw_vol, vol)
    loads[1].wait()
    bins = q_of(dot(mix, vol[0]), dot(mix, vol[1])).astype(BF16)
    spread(footprints(bins), tw, outbox.at[0])
    loads[2].wait()
    view_slab(raw_ds, ds)
    loads[3].wait()
    view_slab(raw_sino, sino)
    loads[4].wait()
    slab(raw_cvol, cvol)
    loads[5].wait()
    view_slab(raw_cd, cd)
    forward_weights(wdi, fdi, 48)
    forward_weights(wdo, fdo, 32)
    forward_weights(wpi, fpi, 48)
    forward_weights(wpo, fpo, 32)
    adjoint_weights(wpo, apo, 32)
    adjoint_weights(wpi, api, 48)
    adjoint_weights(wdo, ado, 32)
    adjoint_weights(wdi, adi, 48)
    pl.semaphore_wait(barrier, n - 1)
    exchange(outbox.at[0], inbox.at[0], 0)
    ds_copies = halo(ds, ds_h, OFFS, 0)
    si_copies = halo(sino, si_h, OFFS, 4)
    def fill_views(rows, own, others, first):
        for z in range(2):
            fill(rows, 2, z, first, own[z * channels : (z + 1) * channels, :])
        for slot, view in enumerate((0, 1, 3, 4)):
            for z in range(2):
                fill(rows, view, z, first, others[slot, z * channels : (z + 1) * channels, :])

    for copy in ds_copies:
        copy.wait_recv()
    fill_views(s_d, ds, ds_h, 0)
    for copy in si_copies:
        copy.wait_recv()

    all_of(inbox.at[0], 0).wait_recv()
    windows = gathered(inbox.at[0], pc, columns)
    pr_own[...] = jnp.concatenate(windows, axis=1).astype(BF16)
    pr_copies = halo(pr_own, pr_h, OFFS, 8)
    vol_copies = halo(vol, vol_h, (-1, 1), 12)
    cvol_copies = halo(cvol, cvol_h, (-1, 1), 14)

    def fill_tail(view, projected, measured):
        for z in range(2):
            block = jnp.concatenate(
                [
                    projected[z * 4 : z * 4 + 4].astype(F32),
                    measured[z * 4 : z * 4 + 4].astype(F32),
                    jnp.zeros((8, width), F32),
                ],
                axis=0,
            ).astype(BF16)
            fill(s_d, view, z, channels, block)

    fill_tail(2, pr_own[...], sino[...])
    for copy in pr_copies:
        copy.wait_recv()
    for slot, view in enumerate((0, 1, 3, 4)):
        fill_tail(view, pr_h[slot], si_h[slot])

    bias_di = column_of(bdi)

    @pl.loop(0, 3)
    def _(v):
        pre = dot(fdi[...], taken(s_d, v)) + bias_di
        dpre[v] = pre
        hidden = (pre * sigmoid(pre)).astype(BF16)
        for z in range(2):
            fill(s_dh, v, z, 0, hidden[z * channels : (z + 1) * channels])

    update = dot(fdo[...], taken(s_dh, 0)) + column_of(bdo)
    fresh = (ds[...].astype(F32) + update).astype(BF16)
    nd[...] = fresh

    def bins_of(block, stride, first):
        return jnp.concatenate(
            [block[first : first + 4], block[stride + first : stride + first + 4]], axis=0
        )

    def parts_of(signal):
        return [signal[:, c * UW : (c + 1) * UW] for c in range(columns)]

    spread(parts_of(bins_of(fresh.astype(F32), channels, 0)), pc, outbox.at[1])
    exchange(outbox.at[1], inbox.at[1], 1)
    cd_copies = halo(cd, cd_h, OFFS, 16)

    low_in = jnp.where(me > 0, 1.0, 0.0).astype(F32)
    high_in = jnp.where(me < n - 1, 1.0, 0.0).astype(F32)

    def fill_rows(rows, own, others):
        for y in range(2):
            for z in range(2):
                part = slice(z * channels, (z + 1) * channels)
                fill(rows, 2 + y, z, 0, own[y, part, :])
                fill(rows, y, z, 0, (others[0, y, part, :].astype(F32) * low_in).astype(BF16))
                fill(rows, 4 + y, z, 0, (others[1, y, part, :].astype(F32) * high_in).astype(BF16))

    for copy in cvol_copies:
        copy.wait_recv()
    fill_rows(s_c, cvol, cvol_h)

    @pl.loop(0, 4)
    def _(r):
        hgrad[r] = dot(apo[...], taken(s_c, r))

    for copy in vol_copies:
        copy.wait_recv()
    fill_rows(s_p, vol, vol_h)

    all_of(inbox.at[1], 1).wait_recv()
    summed = tile_sums(gathered(inbox.at[1], tw, tables))
    bp_own[...] = summed.astype(BF16)
    bp_copies = halo(bp_own, bp_h, (-1, 1), 20)

    def fill_back(row, block):
        for z in range(2):
            part = jnp.concatenate(
                [block[z * 4 : z * 4 + 4], jnp.zeros((12, width), F32)], axis=0
            ).astype(BF16)
            fill(s_p, row, z, channels, part)

    own_back = bp_own[...].astype(F32)
    for y in range(2):
        fill_back(2 + y, own_back[:, y * width : (y + 1) * width])
    for copy in bp_copies:
        copy.wait_recv()
    low_back = bp_h[0].astype(F32) * low_in
    high_back = bp_h[1].astype(F32) * high_in
    for y in range(2):
        fill_back(y, low_back[:, y * width : (y + 1) * width])
        fill_back(4 + y, high_back[:, y * width : (y + 1) * width])

    bias_pi = column_of(bpi)

    @pl.loop(0, 4)
    def _(r):
        pre = dot(fpi[...], taken(s_p, r)) + bias_pi
        ppre[r] = pre
        inside = jnp.where(r == 0, low_in, jnp.where(r == 3, high_in, 1.0))
        s = sigmoid(pre)
        grad = (hgrad[r] * (s * (1.0 + pre * (1.0 - s))) * inside).astype(BF16)
        for z in range(2):
            fill(s_pg, r, z, 0, grad[z * channels : (z + 1) * channels])

    for r in range(2):
        ingrad[r] = dot(api[...], taken(s_pg, r))
    back = q_of(bins_of(ingrad[0], 48, channels), bins_of(ingrad[1], 48, channels)).astype(BF16)
    spread(footprints(back), tw, outbox.at[2])
    exchange(outbox.at[2], inbox.at[2], 2)

    @pl.loop(0, 4)
    def _(r):
        pre = ppre[r]
        inside = jnp.where(r == 0, low_in, jnp.where(r == 3, high_in, 1.0))
        hidden = (pre * sigmoid(pre) * inside).astype(BF16)
        for z in range(2):
            fill(s_ph, r, z, 0, hidden[z * channels : (z + 1) * channels])

    def packed(inner, outer, side):
        for k in range(9):
            rsum[k * 40 : (k + 1) * 40, :] = inner[k * 48 : k * 48 + 40]
        rsum[360:648, :] = outer
        lane = lax.broadcasted_iota(jnp.int32, (160, LANES), 1)
        tail = rsum[488:648, :]
        for i in range(3):
            moved = tail if i == 3 else pltpu.roll(tail, 96 - 32 * i, 1)
            pack[i * 160 : (i + 1) * 160, :] = jnp.where(
                lane < 96, rsum[i * 160 : (i + 1) * 160, :], moved
            )
        pack[480:488, :] = rsum[480:488, :]
        pack[488:512, :] = jnp.zeros((24, LANES), F32)
        px_out[side] = pack[pl.ds(other_half, 256), :].reshape(chips, chunk, LANES)
        return swap(px_out.at[side], px_in.at[side], 8 + side)

    own_half = pl.multiple_of(core * 256, 256)
    other_half = pl.multiple_of(256 - core * 256, 256)

    def chip_sum(side, copy):
        copy.wait_recv()
        own = pack[pl.ds(own_half, 256), :].reshape(chips, chunk, LANES)
        rs_out[side] = (own + px_in[side]).astype(BF16)
        lanes(rs_out.at[side], rs_in.at[side], 4 + side, False)

    def own_rows(rows, y):
        return jnp.concatenate([rows[y, 0, 1], rows[y, 1, 1]], axis=0)

    half_p = packed(
        weight_sum(s_p, 1, [own_rows(s_pg, 1), own_rows(s_pg, 2)]),
        weight_sum(s_ph, 0, [cvol[0], cvol[1]]),
        0,
    )
    for r in range(2):
        change = dot(fpo[...], taken(s_ph, r)) + column_of(bpo)
        nv[r] = (vol[r].astype(F32) + change).astype(BF16)

    chip_sum(0, half_p)
    for copy in cd_copies:
        copy.wait_recv()

    def reduced(side):
        all_of(rs_in.at[side], 4 + side).wait_recv()

        def step(t, total):
            return total + rs_in[side, t].astype(F32)

        total = lax.fori_loop(0, chips, step, jnp.zeros((chunk, LANES), F32), unroll=4)
        ag_own[side] = total.astype(BF16)
        lanes(ag_own.at[side], ag_in.at[side, core], 6 + side, True)

    all_of(inbox.at[2], 2).wait_recv()
    toward = jnp.concatenate(gathered(inbox.at[2], pc, columns), axis=1)
    own_cot = cd[...].astype(F32)
    dtotal[...] = own_cot
    dtotal[0:4, :] = own_cot[0:4] + toward[0:4]
    dtotal[channels : channels + 4, :] = own_cot[channels : channels + 4] + toward[4:8]
    dc_own[...] = bins_of(dtotal[...], channels, 0).astype(BF16)
    dc_copies = halo(dc_own, dc_h, OFFS, 22)
    own_total = dtotal[...].astype(BF16)
    for z in range(2):
        fill(s_dc, 2, z, 0, own_total[z * channels : (z + 1) * channels])
    reduced(0)
    for copy in dc_copies:
        copy.wait_recv()
    for slot, view in enumerate((0, 1, 3, 4)):
        for z in range(2):
            block = jnp.concatenate(
                [
                    dc_h[slot, z * 4 : z * 4 + 4, :].astype(F32),
                    cd_h[slot, z * channels + 4 : (z + 1) * channels, :].astype(F32),
                ],
                axis=0,
            ).astype(BF16)
            fill(s_dc, view, z, 0, block)

    @pl.loop(0, 3)
    def _(v):
        pre = dpre[v]
        s = sigmoid(pre)
        grad = (dot(ado[...], taken(s_dc, v)) * (s * (1.0 + pre * (1.0 - s)))).astype(BF16)
        for z in range(2):
            fill(s_dpg, v, z, 0, grad[z * channels : (z + 1) * channels])

    half_d = packed(
        weight_sum(s_d, 1, [own_rows(s_dpg, 1)]),
        weight_sum(s_dh, 0, [own_total]),
        1,
    )
    dhg[...] = dot(adi[...], taken(s_dpg, 0))
    spread(parts_of(bins_of(dhg[...], 48, channels).astype(BF16).astype(F32)), pc, outbox.at[3])
    chip_sum(1, half_d)
    exchange(outbox.at[3], inbox.at[3], 3)
    for z in range(2):
        part = slice(z * channels, (z + 1) * channels)
        dg[part, :] = (dtotal[part, :] + dhg[z * 48 : z * 48 + channels, :]).astype(BF16)

    reduced(1)
    all_of(inbox.at[3], 3).wait_recv()
    final = tile_sums(gathered(inbox.at[3], tw, tables))
    high = final.astype(BF16)
    low = (final - high.astype(F32)).astype(BF16)
    both = jnp.concatenate([high.astype(F32), low.astype(F32)], axis=0).astype(BF16)
    for y in range(2):
        mixed = dot_tn(mix_twice, both[:, y * width : (y + 1) * width])
        for z in range(2):
            part = slice(z * channels, (z + 1) * channels)
            vg[y, part, :] = (
                cvol[y, part, :].astype(F32)
                + ingrad[y, z * 48 : z * 48 + channels, :]
                + mixed[part]
            ).astype(BF16)

    swaps = []
    for side in range(2):
        all_of(ag_in.at[side, core], 6 + side).wait_recv()
        swaps.append(swap(ag_in.at[side, core], ag_in.at[side, core], 10 + side))
    for side, result in enumerate((gp, gd)):
        swaps[side].wait_recv()
        result[...] = ag_in[side].reshape(result.shape)

    for phase in range(4):
        all_of(inbox.at[phase], phase).wait_send()
    for side in range(2):
        all_of(rs_in.at[side], 4 + side).wait_send()
        all_of(ag_in.at[side, core], 6 + side).wait_send()
    for copy in halos:
        copy.wait_send()


def finish(nv, nd, vg, dg, gp, gd, new_volume, new_dual, volume_grad, dual_grad, *rest):
    grads, (wide, tall) = rest[:4], rest[4:]
    channels = new_dual.shape[0]
    width = new_dual.shape[2]

    for source, target in ((nv, new_volume), (vg, volume_grad)):
        for z in range(2):
            for y in range(2):
                merged(wide, y, source[y, z * channels : (z + 1) * channels, :])
            target[:, z] = rows_from(wide).reshape(channels, 2, width).astype(BF16)
    for source, target in ((nd, new_dual), (dg, dual_grad)):
        for z in range(2):
            merged(wide, z, source[z * channels : (z + 1) * channels, :])
        target[...] = rows_from(wide).reshape(channels, 2, width).astype(BF16)

    for side, packed in enumerate((gp, gd)):
        tall[0:488, :] = packed[0:488, :].astype(F32)
        lane = lax.broadcasted_iota(jnp.int32, (160, LANES), 1)
        rows = jnp.zeros((160, LANES), F32)
        for i in range(3):
            block = packed[i * 160 : (i + 1) * 160, :].astype(F32)
            rows = jnp.where(lane // 32 == i, pltpu.roll(block, 32 * (i + 1), 1), rows)
        tall[488:648, :] = rows
        tall[648:, :] = jnp.zeros((tall.shape[0] - 648, LANES), F32)
        flat = tall[...].T
        for i in range(3):
            part = flat[i * 32 : (i + 1) * 32]
            for k in range(9):
                inner, outer = grads[2 * side], grads[2 * side + 1]
                inner[9 * i + k] = part[:, k * 40 : k * 40 + inner.shape[2]]
                outer[9 * i + k] = part[:, 360 + k * 32 : 360 + k * 32 + outer.shape[2]]


def shards(
    n,
    volume,
    dual_state,
    sinogram,
    cot_volume,
    cot_dual,
    basis_table,
    bin_energy,
    footprint_table,
    hit_tile,
    hit_table,
    hit_column,
    hit_count,
    primal_inner,
    primal_inner_bias,
    primal_outer,
    primal_outer_bias,
    dual_inner,
    dual_inner_bias,
    dual_outer,
    dual_outer_bias,
):
    channels, slices, row_count, width = volume.shape
    bin_count = sinogram.shape[0]
    columns = width // UW
    tables = footprint_table.shape[0]
    both = slices * channels

    chunk = 512 // n
    vmem = pl.BlockSpec(memory_space=pltpu.VMEM)
    smem = pl.BlockSpec(memory_space=pltpu.SMEM)
    shape = jax.ShapeDtypeStruct

    def rows_of(y, c):
        return pltpu.VMEM((y, 2, 3, c, width), BF16)

    any_space = pl.BlockSpec(memory_space=pl.ANY)
    messages = (n, slices * bin_count, UW)
    new_volume, new_dual, volume_grad, dual_grad, packed_primal, packed_dual = pl.pallas_call(
        functools.partial(kernel, n),
        out_shape=(
            shape((row_count, both, width), BF16),
            shape((both, width), BF16),
            shape((row_count, both, width), BF16),
            shape((both, width), BF16),
            shape((n * chunk, LANES), BF16),
            shape((n * chunk, LANES), BF16),
        ),
        in_specs=[smem] + [any_space] * 5 + [vmem, any_space] + [vmem] * 12,
        out_specs=(vmem,) * 6,
        scratch_shapes=[
            pltpu.VMEM(volume.shape, BF16),
            pltpu.VMEM(volume.shape, BF16),
            pltpu.VMEM((channels, slices, width), BF16),
            pltpu.VMEM((channels, slices, width), BF16),
            pltpu.VMEM((bin_count, slices, width), BF16),
            pltpu.VMEM(footprint_table.shape, BF16),
            pltpu.VMEM((width // LANES, both, LANES), F32),
            pltpu.VMEM((row_count, both, width), BF16),
            pltpu.VMEM((row_count, both, width), BF16),
            pltpu.VMEM((both, width), BF16),
            pltpu.VMEM((both, width), BF16),
            pltpu.VMEM((slices * bin_count, width), BF16),
            pltpu.VMEM((tables, n, LANES), F32),
            pltpu.VMEM((columns, n, LANES), F32),
            pltpu.VMEM((64, 18 * 48), BF16),
            pltpu.VMEM((64, 18 * 32), BF16),
            pltpu.VMEM((64, 18 * 48), BF16),
            pltpu.VMEM((64, 18 * 32), BF16),
            pltpu.VMEM((96, 18 * 32), BF16),
            pltpu.VMEM((64, 18 * 32), BF16),
            pltpu.VMEM((96, 18 * 32), BF16),
            pltpu.VMEM((64, 18 * 32), BF16),
            rows_of(5, 48),
            rows_of(3, 32),
            rows_of(6, 48),
            rows_of(4, 32),
            rows_of(6, 32),
            rows_of(4, 32),
            rows_of(5, 32),
            rows_of(3, 32),
            pltpu.VMEM((4, both, width), BF16),
            pltpu.VMEM((4, 8, width), BF16),
            pltpu.VMEM((4, 8, width), BF16),
            pltpu.VMEM((2, row_count, both, width), BF16),
            pltpu.VMEM((2, row_count, both, width), BF16),
            pltpu.VMEM((4, both, width), BF16),
            pltpu.VMEM((2, 8, row_count * width), BF16),
            pltpu.VMEM((4, 8, width), BF16),
            pltpu.VMEM((8, width), BF16),
            pltpu.VMEM((8, row_count * width), BF16),
            pltpu.VMEM((8, width), BF16),
            pltpu.VMEM((3, both, width), F32),
            pltpu.VMEM((4, both, width), F32),
            pltpu.VMEM((4, both, width), F32),
            pltpu.VMEM((2, 96, width), F32),
            pltpu.VMEM((both, width), F32),
            pltpu.VMEM((96, width), F32),
            pltpu.VMEM((648, LANES), F32),
            pltpu.VMEM((512, LANES), F32),
            pltpu.VMEM((4,) + messages, BF16),
            pltpu.VMEM((4,) + messages, BF16),
            pltpu.VMEM((2, n // 2, chunk, LANES), F32),
            pltpu.VMEM((2, n // 2, chunk, LANES), F32),
            pltpu.VMEM((2, n // 2, chunk, LANES), BF16),
            pltpu.VMEM((2, n // 2, chunk, LANES), BF16),
            pltpu.VMEM((2, chunk, LANES), BF16),
            pltpu.VMEM((2, 2, n // 2, chunk, LANES), BF16),
            pltpu.SemaphoreType.DMA((6,)),
            pltpu.SemaphoreType.DMA((12,)),
            pltpu.SemaphoreType.DMA((12,)),
            pltpu.SemaphoreType.DMA((26,)),
            pltpu.SemaphoreType.DMA((26,)),
        ],
        compiler_params=pltpu.CompilerParams(
            collective_id=0, has_side_effects=True, vmem_limit_bytes=60 * 1024 * 1024
        ),
    )(
        bin_energy,
        volume,
        dual_state.reshape(channels, slices, width),
        sinogram.reshape(bin_count, slices, width),
        cot_volume,
        cot_dual.reshape(channels, slices, width),
        basis_table,
        footprint_table,
        hit_tile.T,
        hit_table.T,
        hit_column.T,
        hit_count.reshape(1, n),
        primal_inner,
        primal_outer,
        dual_inner,
        dual_outer,
        *(
            b.reshape(1, channels)
            for b in (primal_inner_bias, primal_outer_bias, dual_inner_bias, dual_outer_bias)
        ),
    )
    new_volume, new_dual, volume_grad, dual_grad, *gradients = pl.pallas_call(
        finish,
        out_shape=(
            shape(volume.shape, BF16),
            shape((channels, slices, width), BF16),
            shape(volume.shape, BF16),
            shape((channels, slices, width), BF16),
            *(
                shape(w.shape, F32)
                for w in (primal_inner, primal_outer, dual_inner, dual_outer)
            ),
        ),
        in_specs=[vmem] * 6,
        out_specs=(vmem,) * 8,
        scratch_shapes=[
            pltpu.VMEM((width // LANES, both, LANES), F32),
            pltpu.VMEM((768, LANES), F32),
        ],
    )(new_volume, new_dual, volume_grad, dual_grad, packed_primal, packed_dual)
    return (
        new_volume,
        new_dual.reshape(dual_state.shape),
        volume_grad,
        dual_grad.reshape(dual_state.shape),
        *gradients,
    )


def solution(mesh):
    part = P(None, "parts", AXIS, None)
    return jax.shard_map(
        functools.partial(shards, mesh.shape[AXIS]),
        mesh=mesh,
        in_specs=(part,) * 5 + (P(),) * 15,
        out_specs=(part,) * 4 + (P("parts", None, None),) * 4,
        check_vma=False,
    )
```

```python
import functools

import jax
import jax.numpy as jnp
from jax import lax
from jax.experimental import pallas as pl
from jax.experimental.pallas import tpu as pltpu
from jax.sharding import PartitionSpec as P

F32 = jnp.float32
BF16 = jnp.bfloat16
MESH = pl.DeviceIdType.MESH
AXIS = "view"
UW = 128
LANES = 128
OFFS = (-2, -1, 1, 2)


def dot(a, b):
    return jnp.dot(a, b, preferred_element_type=F32)


def dot_tn(a, b):
    return lax.dot_general(a, b, (((0,), (0,)), ((), ())), preferred_element_type=F32)


def dot_nt(a, b):
    return lax.dot_general(a, b, (((1,), (1,)), ((), ())), preferred_element_type=F32)


def sigmoid(a):
    return 1.0 / (1.0 + jnp.exp(-a))


def padded(piece, width):
    if piece.shape[1] == width:
        return piece
    return jnp.concatenate(
        [piece, jnp.zeros((piece.shape[0], width - piece.shape[1]), piece.dtype)], axis=1
    )


def forward_weights(weight, target, width):
    outs = weight.shape[1]
    for zo in range(2):
        pieces = []
        for j in range(3):
            for zi in range(2):
                for l in range(3):
                    tap = 9 * (zi - zo + 1) + 3 * j + l
                    pieces.append(padded(weight[tap].astype(F32), width))
        target[zo * outs : (zo + 1) * outs, :] = jnp.concatenate(pieces, axis=1).astype(BF16)


def adjoint_weights(weight, target, width):
    rows = []
    for j in range(3):
        for zi in range(2):
            for l in range(3):
                pair = []
                for zo in range(2):
                    tap = 26 - (9 * (zi - zo + 1) + 3 * j + l)
                    pair.append(padded(weight[tap].astype(F32), width))
                rows.append(padded(jnp.concatenate(pair, axis=1), LANES))
    tall = jnp.concatenate(rows, axis=0)
    target[...] = tall.T[: 2 * width].astype(BF16)


def shifted(block):
    wide = block.astype(F32)
    last = block.shape[1] - 1
    lane = lax.broadcasted_iota(jnp.int32, wide.shape, 1)
    low = jnp.where(lane == 0, 0.0, pltpu.roll(wide, 1, 1)).astype(BF16)
    high = jnp.where(lane == last, 0.0, pltpu.roll(wide, last, 1)).astype(BF16)
    return low, high


def fill(rows, y, z, first, block):
    height = block.shape[0]
    low, high = shifted(block)
    rows[y, z, 0, first : first + height, :] = low
    rows[y, z, 1, first : first + height, :] = block
    rows[y, z, 2, first : first + height, :] = high


def taken(rows, y):
    part = rows[pl.ds(y, 3)]
    return part.reshape(part.shape[0] * part.shape[1] * part.shape[2] * part.shape[3], part.shape[4])


def parted(wide, first, count):
    blocks = [wide[k, pl.ds(first, count, stride=2), :] for k in range(wide.shape[0])]
    return jnp.concatenate(blocks, axis=1).astype(BF16)


def merged(wide, first, block):
    for k in range(wide.shape[0]):
        wide[k, pl.ds(first, block.shape[0], stride=2), :] = block[
            :, k * LANES : (k + 1) * LANES
        ].astype(F32)


def rows_from(wide):
    return jnp.concatenate([wide[k] for k in range(wide.shape[0])], axis=1)


def weight_sum(rows, first, cots):
    total = None
    for r, cot in enumerate(cots):
        high, low = cot[32:64], cot[0:32]
        none = jnp.zeros_like(low)
        for zi in range(2):
            spread = [high, low, none, none] if zi == 0 else [none, high, low, none]
            part = rows[first + r : first + r + 3, zi]
            part = part.reshape(part.shape[0] * part.shape[1] * part.shape[2], part.shape[3])
            term = dot_nt(part, jnp.concatenate(spread, axis=0))
            total = term if total is None else total + term
    return total


def kernel(
    n,
    energy,
    volume,
    dual_state,
    sinogram,
    cot_volume,
    cot_dual,
    basis,
    footprint_table,
    tiles,
    kinds,
    places,
    counts,
    wpi,
    wpo,
    wdi,
    wdo,
    bpi,
    bpo,
    bdi,
    bdo,
    nv,
    nd,
    vg,
    dg,
    gp,
    gd,
    raw_vol,
    raw_cvol,
    raw_ds,
    raw_cd,
    raw_sino,
    table,
    wide,
    vol,
    cvol,
    ds,
    cd,
    sino,
    tw,
    pc,
    fpi,
    fpo,
    fdi,
    fdo,
    api,
    apo,
    adi,
    ado,
    s_d,
    s_dh,
    s_p,
    s_ph,
    s_c,
    s_pg,
    s_dc,
    s_dpg,
    ds_h,
    si_h,
    pr_h,
    vol_h,
    cvol_h,
    cd_h,
    bp_h,
    dc_h,
    pr_own,
    bp_own,
    dc_own,
    dpre,
    ppre,
    hgrad,
    ingrad,
    dtotal,
    dhg,
    rsum,
    pack,
    outbox,
    inbox,
    px_out,
    px_in,
    rs_out,
    rs_in,
    ag_own,
    ag_in,
    load,
    send,
    recv,
    hsend,
    hrecv,
):
    me = lax.axis_index(AXIS)
    chips = n // 2
    chip = me // 2
    core = me % 2
    partner = me + 1 - 2 * core
    channels = ds.shape[0] // 2
    width = ds.shape[1]
    columns = width // UW
    tables = table.shape[0]
    chunk = ag_own.shape[1]

    def to(offset):
        return lax.rem(me + offset + n, n)

    def far_first(k, count):
        half = lax.shift_right_logical(k, 1)
        return jnp.where(lax.bitwise_and(k, 1) == 0, count // 2 + half, count // 2 - 1 - half)

    def wrapped(index, count):
        return jnp.where(index >= count, index - count, index)

    def steps(low, high):
        return pl.loop(low, high, unroll=7 if (high - low) % 7 == 0 else 1)

    barrier = pltpu.get_barrier_semaphore()

    @steps(0, n - 1)
    def _(k):
        peer = wrapped(me + far_first(k, n), n)
        pl.semaphore_signal(barrier, inc=1, device_id={AXIS: peer}, device_id_type=MESH)

    loads = [
        pltpu.make_async_copy(source, target, load.at[i])
        for i, (source, target) in enumerate(
            (
                (volume, raw_vol),
                (footprint_table, table),
                (dual_state, raw_ds),
                (sinogram, raw_sino),
                (cot_volume, raw_cvol),
                (cot_dual, raw_cd),
            )
        )
    ]
    for copy in loads:
        copy.start()

    def exchange(source, target, phase, low=0, high=n - 1):
        @steps(low, high)
        def _(k):
            peer = wrapped(me + far_first(k, n), n)
            pltpu.make_async_remote_copy(
                src_ref=source.at[peer],
                dst_ref=target.at[me],
                send_sem=send.at[phase],
                recv_sem=recv.at[phase],
                device_id={AXIS: peer},
                device_id_type=MESH,
            ).start()

        if low == 0:
            target[me] = source[me]

    apart = 4
    members = chips // apart

    def slot_of(there):
        return (there % apart) * members + there // apart

    own_slot = slot_of(chip)

    def lanes(source, target, phase, same):
        @steps(0, chips - 1)
        def _(k):
            there = wrapped(chip + far_first(k, chips), chips)
            pltpu.make_async_remote_copy(
                src_ref=source if same else source.at[slot_of(there)],
                dst_ref=target.at[own_slot],
                send_sem=send.at[phase],
                recv_sem=recv.at[phase],
                device_id={AXIS: 2 * there + core},
                device_id_type=MESH,
            ).start()

        target[own_slot] = source[...] if same else source[own_slot]

    def class_far(source, target, phase):
        @steps(0, members - 1)
        def _(k):
            there = wrapped(chip + apart * far_first(k, members), chips)
            pltpu.make_async_remote_copy(
                src_ref=source,
                dst_ref=target.at[own_slot],
                send_sem=send.at[phase],
                recv_sem=recv.at[phase],
                device_id={AXIS: 2 * there + core},
                device_id_type=MESH,
            ).start()

        target[own_slot] = source[...]

    def class_near(target, phase):
        own = target.at[pl.ds((chip % apart) * members, members)]
        for step in (2, 1, chips - 1):
            pltpu.make_async_remote_copy(
                src_ref=own,
                dst_ref=own,
                send_sem=send.at[phase],
                recv_sem=recv.at[phase],
                device_id={AXIS: 2 * wrapped(chip + step, chips) + core},
                device_id_type=MESH,
            ).start()

    def all_of(target, phase, count=None):
        part = target.at[pl.ds(0, count or target.shape[0] - 1)]
        return pltpu.make_async_remote_copy(
            src_ref=part,
            dst_ref=part,
            send_sem=send.at[phase],
            recv_sem=recv.at[phase],
            device_id={AXIS: to(1)},
            device_id_type=MESH,
        )

    halos = []

    def halo(source, target, offsets, base):
        copies = []
        for slot, offset in enumerate(offsets):
            there = len(offsets) - 1 - slot
            copies.append(
                pltpu.make_async_remote_copy(
                    src_ref=source,
                    dst_ref=target.at[there],
                    send_sem=hsend.at[base + there],
                    recv_sem=hrecv.at[base + there],
                    device_id={AXIS: to(offset)},
                    device_id_type=MESH,
                )
            )
        for copy in copies:
            copy.start()
        halos.extend(copies)
        return copies

    def swap(source, target, phase):
        copy = pltpu.make_async_remote_copy(
            src_ref=source,
            dst_ref=target,
            send_sem=send.at[phase],
            recv_sem=recv.at[phase],
            device_id={AXIS: partner},
            device_id_type=MESH,
        )
        copy.start()
        halos.append(copy)
        return copy

    def footprints(q):
        return [dot(q, table[o]) for o in range(tables)]

    def spread(values, scale, target):
        @pl.loop(0, n, unroll=4)
        def _(b):
            total = scale[0, pl.ds(b, 1), :] * values[0]
            for o in range(1, len(values)):
                total = total + scale[o, pl.ds(b, 1), :] * values[o]
            target[b] = total.astype(BF16)

    def gathered(source, scale, count):
        def step(t, totals):
            block = source[t].astype(F32)
            return tuple(totals[c] + scale[c, pl.ds(t, 1), :] * block for c in range(count))

        start = tuple(jnp.zeros(source.shape[1:], F32) for _ in range(count))
        return lax.fori_loop(0, n, step, start, unroll=4)

    def q_of(y0, y1):
        return jnp.concatenate([y0, y1], axis=1)

    def tile_sums(groups):
        total = None
        for o in range(tables):
            high = groups[o].astype(BF16)
            low = (groups[o] - high.astype(F32)).astype(BF16)
            term = dot_nt(jnp.concatenate([high, low], axis=0), table[o])
            total = term if total is None else total + term
        return total[0:8] + total[8:16]

    entries = tiles.shape[0]
    entry = lax.broadcasted_iota(jnp.int32, (entries, n), 0)
    lane = lax.broadcasted_iota(jnp.int32, (entries, n), 1)
    ones = jnp.ones((entries, LANES), BF16)

    def flags(mask):
        return dot_tn(jnp.where(mask, 1.0, 0.0).astype(BF16), ones)

    tile, kind, place = tiles[...], kinds[...], places[...]
    live = entry < counts[...]
    for o in range(tables):
        tw[o] = flags(live & (tile == me) & (kind == o))

    def own_column(values):
        return jnp.sum(jnp.where(lane == me, values, 0.0), axis=1, keepdims=True)

    own_live = own_column(jnp.where(live, 1.0, 0.0))
    own_tile = own_column(tile.astype(F32))
    own_place = own_column(place.astype(F32))
    hit = (own_tile == lane.astype(F32)) & (own_live > 0.5)
    for c in range(columns):
        pc[c] = flags(hit & (own_place == float(c)))

    row = lax.broadcasted_iota(jnp.int32, (8, 8), 0)
    col = lax.broadcasted_iota(jnp.int32, (8, 8), 1)
    chosen = jnp.zeros((8, 8), F32)
    for b in range(4):
        chosen = chosen + jnp.where((row % 4 == b) & (col == energy[b]), 1.0, 0.0)
    mixing = dot(chosen.astype(BF16), basis[...])
    both_z = jnp.concatenate([mixing, mixing], axis=1)
    row = lax.broadcasted_iota(jnp.int32, both_z.shape, 0)
    col = lax.broadcasted_iota(jnp.int32, both_z.shape, 1)
    mix_wide = jnp.where(row // 4 == col // channels, both_z, 0.0)
    mix = mix_wide.astype(BF16)
    mix_twice = jnp.concatenate([mix_wide, mix_wide], axis=0).astype(BF16)

    def column_of(bias):
        row = lax.broadcasted_iota(jnp.int32, (2 * channels, channels), 0)
        col = lax.broadcasted_iota(jnp.int32, (2 * channels, channels), 1)
        return jnp.sum(jnp.where(row % channels == col, bias[...], 0.0), axis=1, keepdims=True)

    def slab(source, target):
        for z in range(2):
            part = source[:, z].astype(F32).reshape(2 * channels, width)
            for k in range(width // LANES):
                wide[k] = part[:, k * LANES : (k + 1) * LANES]
            for y in range(2):
                target[y, z * channels : (z + 1) * channels, :] = parted(wide, y, channels)

    def view_slab(source, target):
        count = source.shape[0]
        part = source[...].astype(F32).reshape(2 * count, width)
        for k in range(width // LANES):
            wide[k, 0 : 2 * count, :] = part[:, k * LANES : (k + 1) * LANES]
        if count % 16 == 0:
            for z in range(2):
                target[z * count : (z + 1) * count, :] = parted(wide, z, count)
        else:
            target[...] = jnp.concatenate(
                [parted(wide, z, count).astype(F32) for z in range(2)], axis=0
            ).astype(BF16)

    loads[0].wait()
    slab(raw_vol, vol)
    loads[1].wait()
    bins = q_of(dot(mix, vol[0]), dot(mix, vol[1])).astype(BF16)
    spread(footprints(bins), tw, outbox.at[0])
    loads[2].wait()
    view_slab(raw_ds, ds)
    loads[3].wait()
    view_slab(raw_sino, sino)
    loads[4].wait()
    slab(raw_cvol, cvol)
    loads[5].wait()
    view_slab(raw_cd, cd)
    forward_weights(wdi, fdi, 48)
    forward_weights(wdo, fdo, 32)
    forward_weights(wpi, fpi, 48)
    forward_weights(wpo, fpo, 32)
    adjoint_weights(wpo, apo, 32)
    adjoint_weights(wpi, api, 48)
    adjoint_weights(wdo, ado, 32)
    adjoint_weights(wdi, adi, 48)
    pl.semaphore_wait(barrier, n - 1)
    exchange(outbox.at[0], inbox.at[0], 0)
    ds_copies = halo(ds, ds_h, OFFS, 0)
    si_copies = halo(sino, si_h, OFFS, 4)
    def fill_views(rows, own, others, first):
        for z in range(2):
            fill(rows, 2, z, first, own[z * channels : (z + 1) * channels, :])
        for slot, view in enumerate((0, 1, 3, 4)):
            for z in range(2):
                fill(rows, view, z, first, others[slot, z * channels : (z + 1) * channels, :])

    for copy in ds_copies:
        copy.wait_recv()
    fill_views(s_d, ds, ds_h, 0)
    for copy in si_copies:
        copy.wait_recv()

    all_of(inbox.at[0], 0).wait_recv()
    windows = gathered(inbox.at[0], pc, columns)
    pr_own[...] = jnp.concatenate(windows, axis=1).astype(BF16)
    pr_copies = halo(pr_own, pr_h, OFFS, 8)
    vol_copies = halo(vol, vol_h, (-1, 1), 12)
    cvol_copies = halo(cvol, cvol_h, (-1, 1), 14)

    def fill_tail(view, projected, measured):
        for z in range(2):
            block = jnp.concatenate(
                [
                    projected[z * 4 : z * 4 + 4].astype(F32),
                    measured[z * 4 : z * 4 + 4].astype(F32),
                    jnp.zeros((8, width), F32),
                ],
                axis=0,
            ).astype(BF16)
            fill(s_d, view, z, channels, block)

    fill_tail(2, pr_own[...], sino[...])
    for copy in pr_copies:
        copy.wait_recv()
    for slot, view in enumerate((0, 1, 3, 4)):
        fill_tail(view, pr_h[slot], si_h[slot])

    bias_di = column_of(bdi)

    @pl.loop(0, 3)
    def _(v):
        pre = dot(fdi[...], taken(s_d, v)) + bias_di
        dpre[v] = pre
        hidden = (pre * sigmoid(pre)).astype(BF16)
        for z in range(2):
            fill(s_dh, v, z, 0, hidden[z * channels : (z + 1) * channels])

    update = dot(fdo[...], taken(s_dh, 0)) + column_of(bdo)
    fresh = (ds[...].astype(F32) + update).astype(BF16)
    nd[...] = fresh

    def bins_of(block, stride, first):
        return jnp.concatenate(
            [block[first : first + 4], block[stride + first : stride + first + 4]], axis=0
        )

    def parts_of(signal):
        return [signal[:, c * UW : (c + 1) * UW] for c in range(columns)]

    spread(parts_of(bins_of(fresh.astype(F32), channels, 0)), pc, outbox.at[1])
    exchange(outbox.at[1], inbox.at[1], 1)
    cd_copies = halo(cd, cd_h, OFFS, 16)

    low_in = jnp.where(me > 0, 1.0, 0.0).astype(F32)
    high_in = jnp.where(me < n - 1, 1.0, 0.0).astype(F32)

    def fill_rows(rows, own, others):
        for y in range(2):
            for z in range(2):
                part = slice(z * channels, (z + 1) * channels)
                fill(rows, 2 + y, z, 0, own[y, part, :])
                fill(rows, y, z, 0, (others[0, y, part, :].astype(F32) * low_in).astype(BF16))
                fill(rows, 4 + y, z, 0, (others[1, y, part, :].astype(F32) * high_in).astype(BF16))

    for copy in cvol_copies:
        copy.wait_recv()
    fill_rows(s_c, cvol, cvol_h)

    @pl.loop(0, 4)
    def _(r):
        hgrad[r] = dot(apo[...], taken(s_c, r))

    for copy in vol_copies:
        copy.wait_recv()
    fill_rows(s_p, vol, vol_h)

    all_of(inbox.at[1], 1).wait_recv()
    summed = tile_sums(gathered(inbox.at[1], tw, tables))
    bp_own[...] = summed.astype(BF16)
    bp_copies = halo(bp_own, bp_h, (-1, 1), 20)

    def fill_back(row, block):
        for z in range(2):
            part = jnp.concatenate(
                [block[z * 4 : z * 4 + 4], jnp.zeros((12, width), F32)], axis=0
            ).astype(BF16)
            fill(s_p, row, z, channels, part)

    own_back = bp_own[...].astype(F32)
    for y in range(2):
        fill_back(2 + y, own_back[:, y * width : (y + 1) * width])
    for copy in bp_copies:
        copy.wait_recv()
    low_back = bp_h[0].astype(F32) * low_in
    high_back = bp_h[1].astype(F32) * high_in
    for y in range(2):
        fill_back(y, low_back[:, y * width : (y + 1) * width])
        fill_back(4 + y, high_back[:, y * width : (y + 1) * width])

    bias_pi = column_of(bpi)

    @pl.loop(0, 4)
    def _(r):
        pre = dot(fpi[...], taken(s_p, r)) + bias_pi
        ppre[r] = pre
        inside = jnp.where(r == 0, low_in, jnp.where(r == 3, high_in, 1.0))
        s = sigmoid(pre)
        grad = (hgrad[r] * (s * (1.0 + pre * (1.0 - s))) * inside).astype(BF16)
        for z in range(2):
            fill(s_pg, r, z, 0, grad[z * channels : (z + 1) * channels])

    for r in range(2):
        ingrad[r] = dot(api[...], taken(s_pg, r))
    back = q_of(bins_of(ingrad[0], 48, channels), bins_of(ingrad[1], 48, channels)).astype(BF16)
    spread(footprints(back), tw, outbox.at[2])
    exchange(outbox.at[2], inbox.at[2], 2)

    @pl.loop(0, 4)
    def _(r):
        pre = ppre[r]
        inside = jnp.where(r == 0, low_in, jnp.where(r == 3, high_in, 1.0))
        hidden = (pre * sigmoid(pre) * inside).astype(BF16)
        for z in range(2):
            fill(s_ph, r, z, 0, hidden[z * channels : (z + 1) * channels])

    def packed(inner, outer, side):
        for k in range(9):
            rsum[k * 40 : (k + 1) * 40, :] = inner[k * 48 : k * 48 + 40]
        rsum[360:648, :] = outer
        lane = lax.broadcasted_iota(jnp.int32, (160, LANES), 1)
        tail = rsum[488:648, :]
        for i in range(3):
            moved = tail if i == 3 else pltpu.roll(tail, 96 - 32 * i, 1)
            pack[i * 160 : (i + 1) * 160, :] = jnp.where(
                lane < 96, rsum[i * 160 : (i + 1) * 160, :], moved
            )
        pack[480:488, :] = rsum[480:488, :]
        pack[488:512, :] = jnp.zeros((24, LANES), F32)
        px_out[side] = pack[pl.ds(other_half, 256), :].reshape(chips, chunk, LANES)
        return swap(px_out.at[side], px_in.at[side], 8 + side)

    own_half = pl.multiple_of(core * 256, 256)
    other_half = pl.multiple_of(256 - core * 256, 256)

    def chip_sum(side, copy):
        copy.wait_recv()
        own = pack[pl.ds(own_half, 256), :].reshape(chips, chunk, LANES)
        rs_out[side] = (own + px_in[side]).astype(BF16)

    def own_rows(rows, y):
        return jnp.concatenate([rows[y, 0, 1], rows[y, 1, 1]], axis=0)

    half_p = packed(
        weight_sum(s_p, 1, [own_rows(s_pg, 1), own_rows(s_pg, 2)]),
        weight_sum(s_ph, 0, [cvol[0], cvol[1]]),
        0,
    )
    for r in range(2):
        change = dot(fpo[...], taken(s_ph, r)) + column_of(bpo)
        nv[r] = (vol[r].astype(F32) + change).astype(BF16)

    chip_sum(0, half_p)
    for copy in cd_copies:
        copy.wait_recv()

    def reduced(side):
        all_of(rs_in.at[side], 4 + side).wait_recv()

        def step(t, total):
            return total + rs_in[side, t].astype(F32)

        total = lax.fori_loop(0, chips, step, jnp.zeros((chunk, LANES), F32), unroll=4)
        ag_own[side] = total.astype(BF16)

    all_of(inbox.at[2], 2).wait_recv()
    toward = jnp.concatenate(gathered(inbox.at[2], pc, columns), axis=1)
    own_cot = cd[...].astype(F32)
    dtotal[...] = own_cot
    dtotal[0:4, :] = own_cot[0:4] + toward[0:4]
    dtotal[channels : channels + 4, :] = own_cot[channels : channels + 4] + toward[4:8]
    dc_own[...] = bins_of(dtotal[...], channels, 0).astype(BF16)
    dc_copies = halo(dc_own, dc_h, OFFS, 22)
    lanes(rs_out.at[0], rs_in.at[0], 4, False)
    own_total = dtotal[...].astype(BF16)
    for z in range(2):
        fill(s_dc, 2, z, 0, own_total[z * channels : (z + 1) * channels])
    for copy in dc_copies:
        copy.wait_recv()
    for slot, view in enumerate((0, 1, 3, 4)):
        for z in range(2):
            block = jnp.concatenate(
                [
                    dc_h[slot, z * 4 : z * 4 + 4, :].astype(F32),
                    cd_h[slot, z * channels + 4 : (z + 1) * channels, :].astype(F32),
                ],
                axis=0,
            ).astype(BF16)
            fill(s_dc, view, z, 0, block)

    @pl.loop(0, 3)
    def _(v):
        pre = dpre[v]
        s = sigmoid(pre)
        grad = (dot(ado[...], taken(s_dc, v)) * (s * (1.0 + pre * (1.0 - s)))).astype(BF16)
        for z in range(2):
            fill(s_dpg, v, z, 0, grad[z * channels : (z + 1) * channels])

    half_d = packed(
        weight_sum(s_d, 1, [own_rows(s_dpg, 1)]),
        weight_sum(s_dh, 0, [own_total]),
        1,
    )
    dhg[...] = dot(adi[...], taken(s_dpg, 0))
    spread(parts_of(bins_of(dhg[...], 48, channels).astype(BF16).astype(F32)), pc, outbox.at[3])
    chip_sum(1, half_d)
    lanes(rs_out.at[1], rs_in.at[1], 5, False)
    cut = 7 * ((n - 1) // 14)
    exchange(outbox.at[3], inbox.at[3], 3, 0, cut)
    for z in range(2):
        part = slice(z * channels, (z + 1) * channels)
        dg[part, :] = (dtotal[part, :] + dhg[z * 48 : z * 48 + channels, :]).astype(BF16)
    reduced(0)
    class_far(ag_own.at[0], ag_in.at[0, core], 6)
    exchange(outbox.at[3], inbox.at[3], 3, cut, n - 1)
    reduced(1)
    lanes(ag_own.at[1], ag_in.at[1, core], 7, True)
    all_of(ag_in.at[0, core], 6, members - 1).wait_recv()
    class_near(ag_in.at[0, core], 12)

    all_of(inbox.at[3], 3).wait_recv()
    final = tile_sums(gathered(inbox.at[3], tw, tables))
    high = final.astype(BF16)
    low = (final - high.astype(F32)).astype(BF16)
    both = jnp.concatenate([high.astype(F32), low.astype(F32)], axis=0).astype(BF16)
    for y in range(2):
        mixed = dot_tn(mix_twice, both[:, y * width : (y + 1) * width])
        for z in range(2):
            part = slice(z * channels, (z + 1) * channels)
            vg[y, part, :] = (
                cvol[y, part, :].astype(F32)
                + ingrad[y, z * 48 : z * 48 + channels, :]
                + mixed[part]
            ).astype(BF16)

    all_of(ag_in.at[0, core], 12, 3 * members).wait_recv()
    swaps = [swap(ag_in.at[0, core], ag_in.at[0, core], 10)]
    all_of(ag_in.at[1, core], 7).wait_recv()
    swaps.append(swap(ag_in.at[1, core], ag_in.at[1, core], 11))
    for side, result in enumerate((gp, gd)):
        swaps[side].wait_recv()
        result[...] = ag_in[side].reshape(result.shape)

    for phase in range(4):
        all_of(inbox.at[phase], phase).wait_send()
    for side in range(2):
        all_of(rs_in.at[side], 4 + side).wait_send()
    all_of(ag_in.at[0, core], 6, members - 1).wait_send()
    all_of(ag_in.at[0, core], 12, 3 * members).wait_send()
    all_of(ag_in.at[1, core], 7).wait_send()
    for copy in halos:
        copy.wait_send()


def finish(nv, nd, vg, dg, gp, gd, new_volume, new_dual, volume_grad, dual_grad, *rest):
    grads, (wide, tall) = rest[:4], rest[4:]
    channels = new_dual.shape[0]
    width = new_dual.shape[2]

    for source, target in ((nv, new_volume), (vg, volume_grad)):
        for z in range(2):
            for y in range(2):
                merged(wide, y, source[y, z * channels : (z + 1) * channels, :])
            target[:, z] = rows_from(wide).reshape(channels, 2, width).astype(BF16)
    for source, target in ((nd, new_dual), (dg, dual_grad)):
        for z in range(2):
            merged(wide, z, source[z * channels : (z + 1) * channels, :])
        target[...] = rows_from(wide).reshape(channels, 2, width).astype(BF16)

    for side, packed in enumerate((gp, gd)):
        tall[0:488, :] = packed[0:488, :].astype(F32)
        lane = lax.broadcasted_iota(jnp.int32, (160, LANES), 1)
        rows = jnp.zeros((160, LANES), F32)
        for i in range(3):
            block = packed[i * 160 : (i + 1) * 160, :].astype(F32)
            rows = jnp.where(lane // 32 == i, pltpu.roll(block, 32 * (i + 1), 1), rows)
        tall[488:648, :] = rows
        tall[648:, :] = jnp.zeros((tall.shape[0] - 648, LANES), F32)
        flat = tall[...].T
        for i in range(3):
            part = flat[i * 32 : (i + 1) * 32]
            for k in range(9):
                inner, outer = grads[2 * side], grads[2 * side + 1]
                inner[9 * i + k] = part[:, k * 40 : k * 40 + inner.shape[2]]
                outer[9 * i + k] = part[:, 360 + k * 32 : 360 + k * 32 + outer.shape[2]]


def shards(
    n,
    volume,
    dual_state,
    sinogram,
    cot_volume,
    cot_dual,
    basis_table,
    bin_energy,
    footprint_table,
    hit_tile,
    hit_table,
    hit_column,
    hit_count,
    primal_inner,
    primal_inner_bias,
    primal_outer,
    primal_outer_bias,
    dual_inner,
    dual_inner_bias,
    dual_outer,
    dual_outer_bias,
):
    channels, slices, row_count, width = volume.shape
    bin_count = sinogram.shape[0]
    columns = width // UW
    tables = footprint_table.shape[0]
    both = slices * channels

    chunk = 512 // n
    vmem = pl.BlockSpec(memory_space=pltpu.VMEM)
    smem = pl.BlockSpec(memory_space=pltpu.SMEM)
    shape = jax.ShapeDtypeStruct

    def rows_of(y, c):
        return pltpu.VMEM((y, 2, 3, c, width), BF16)

    any_space = pl.BlockSpec(memory_space=pl.ANY)
    messages = (n, slices * bin_count, UW)
    new_volume, new_dual, volume_grad, dual_grad, packed_primal, packed_dual = pl.pallas_call(
        functools.partial(kernel, n),
        out_shape=(
            shape((row_count, both, width), BF16),
            shape((both, width), BF16),
            shape((row_count, both, width), BF16),
            shape((both, width), BF16),
            shape((n * chunk, LANES), BF16),
            shape((n * chunk, LANES), BF16),
        ),
        in_specs=[smem] + [any_space] * 5 + [vmem, any_space] + [vmem] * 12,
        out_specs=(vmem,) * 6,
        scratch_shapes=[
            pltpu.VMEM(volume.shape, BF16),
            pltpu.VMEM(volume.shape, BF16),
            pltpu.VMEM((channels, slices, width), BF16),
            pltpu.VMEM((channels, slices, width), BF16),
            pltpu.VMEM((bin_count, slices, width), BF16),
            pltpu.VMEM(footprint_table.shape, BF16),
            pltpu.VMEM((width // LANES, both, LANES), F32),
            pltpu.VMEM((row_count, both, width), BF16),
            pltpu.VMEM((row_count, both, width), BF16),
            pltpu.VMEM((both, width), BF16),
            pltpu.VMEM((both, width), BF16),
            pltpu.VMEM((slices * bin_count, width), BF16),
            pltpu.VMEM((tables, n, LANES), F32),
            pltpu.VMEM((columns, n, LANES), F32),
            pltpu.VMEM((64, 18 * 48), BF16),
            pltpu.VMEM((64, 18 * 32), BF16),
            pltpu.VMEM((64, 18 * 48), BF16),
            pltpu.VMEM((64, 18 * 32), BF16),
            pltpu.VMEM((96, 18 * 32), BF16),
            pltpu.VMEM((64, 18 * 32), BF16),
            pltpu.VMEM((96, 18 * 32), BF16),
            pltpu.VMEM((64, 18 * 32), BF16),
            rows_of(5, 48),
            rows_of(3, 32),
            rows_of(6, 48),
            rows_of(4, 32),
            rows_of(6, 32),
            rows_of(4, 32),
            rows_of(5, 32),
            rows_of(3, 32),
            pltpu.VMEM((4, both, width), BF16),
            pltpu.VMEM((4, 8, width), BF16),
            pltpu.VMEM((4, 8, width), BF16),
            pltpu.VMEM((2, row_count, both, width), BF16),
            pltpu.VMEM((2, row_count, both, width), BF16),
            pltpu.VMEM((4, both, width), BF16),
            pltpu.VMEM((2, 8, row_count * width), BF16),
            pltpu.VMEM((4, 8, width), BF16),
            pltpu.VMEM((8, width), BF16),
            pltpu.VMEM((8, row_count * width), BF16),
            pltpu.VMEM((8, width), BF16),
            pltpu.VMEM((3, both, width), F32),
            pltpu.VMEM((4, both, width), F32),
            pltpu.VMEM((4, both, width), F32),
            pltpu.VMEM((2, 96, width), F32),
            pltpu.VMEM((both, width), F32),
            pltpu.VMEM((96, width), F32),
            pltpu.VMEM((648, LANES), F32),
            pltpu.VMEM((512, LANES), F32),
            pltpu.VMEM((4,) + messages, BF16),
            pltpu.VMEM((4,) + messages, BF16),
            pltpu.VMEM((2, n // 2, chunk, LANES), F32),
            pltpu.VMEM((2, n // 2, chunk, LANES), F32),
            pltpu.VMEM((2, n // 2, chunk, LANES), BF16),
            pltpu.VMEM((2, n // 2, chunk, LANES), BF16),
            pltpu.VMEM((2, chunk, LANES), BF16),
            pltpu.VMEM((2, 2, n // 2, chunk, LANES), BF16),
            pltpu.SemaphoreType.DMA((6,)),
            pltpu.SemaphoreType.DMA((13,)),
            pltpu.SemaphoreType.DMA((13,)),
            pltpu.SemaphoreType.DMA((26,)),
            pltpu.SemaphoreType.DMA((26,)),
        ],
        compiler_params=pltpu.CompilerParams(
            collective_id=0, has_side_effects=True, vmem_limit_bytes=60 * 1024 * 1024
        ),
    )(
        bin_energy,
        volume,
        dual_state.reshape(channels, slices, width),
        sinogram.reshape(bin_count, slices, width),
        cot_volume,
        cot_dual.reshape(channels, slices, width),
        basis_table,
        footprint_table,
        hit_tile.T,
        hit_table.T,
        hit_column.T,
        hit_count.reshape(1, n),
        primal_inner,
        primal_outer,
        dual_inner,
        dual_outer,
        *(
            b.reshape(1, channels)
            for b in (primal_inner_bias, primal_outer_bias, dual_inner_bias, dual_outer_bias)
        ),
    )
    new_volume, new_dual, volume_grad, dual_grad, *gradients = pl.pallas_call(
        finish,
        out_shape=(
            shape(volume.shape, BF16),
            shape((channels, slices, width), BF16),
            shape(volume.shape, BF16),
            shape((channels, slices, width), BF16),
            *(
                shape(w.shape, F32)
                for w in (primal_inner, primal_outer, dual_inner, dual_outer)
            ),
        ),
        in_specs=[vmem] * 6,
        out_specs=(vmem,) * 8,
        scratch_shapes=[
            pltpu.VMEM((width // LANES, both, LANES), F32),
            pltpu.VMEM((768, LANES), F32),
        ],
    )(new_volume, new_dual, volume_grad, dual_grad, packed_primal, packed_dual)
    return (
        new_volume,
        new_dual.reshape(dual_state.shape),
        volume_grad,
        dual_grad.reshape(dual_state.shape),
        *gradients,
    )


def solution(mesh):
    part = P(None, "parts", AXIS, None)
    return jax.shard_map(
        functools.partial(shards, mesh.shape[AXIS]),
        mesh=mesh,
        in_specs=(part,) * 5 + (P(),) * 15,
        out_specs=(part,) * 4 + (P("parts", None, None),) * 4,
        check_vma=False,
    )
```

```python
import functools

import jax
import jax.numpy as jnp
from jax import lax
from jax.experimental import pallas as pl
from jax.experimental.pallas import tpu as pltpu
from jax.sharding import PartitionSpec as P

F32 = jnp.float32
BF16 = jnp.bfloat16
MESH = pl.DeviceIdType.MESH
AXIS = "view"
UW = 128
LANES = 128
OFFS = (-2, -1, 1, 2)


def dot(a, b):
    return jnp.dot(a, b, preferred_element_type=F32)


def dot_tn(a, b):
    return lax.dot_general(a, b, (((0,), (0,)), ((), ())), preferred_element_type=F32)


def dot_nt(a, b):
    return lax.dot_general(a, b, (((1,), (1,)), ((), ())), preferred_element_type=F32)


def sigmoid(a):
    return 1.0 / (1.0 + jnp.exp(-a))


def padded(piece, width):
    if piece.shape[1] == width:
        return piece
    return jnp.concatenate(
        [piece, jnp.zeros((piece.shape[0], width - piece.shape[1]), piece.dtype)], axis=1
    )


def forward_weights(weight, target, width):
    outs = weight.shape[1]
    for zo in range(2):
        pieces = []
        for j in range(3):
            for zi in range(2):
                for l in range(3):
                    tap = 9 * (zi - zo + 1) + 3 * j + l
                    pieces.append(padded(weight[tap].astype(F32), width))
        target[zo * outs : (zo + 1) * outs, :] = jnp.concatenate(pieces, axis=1).astype(BF16)


def adjoint_weights(weight, target, width):
    rows = []
    for j in range(3):
        for zi in range(2):
            for l in range(3):
                pair = []
                for zo in range(2):
                    tap = 26 - (9 * (zi - zo + 1) + 3 * j + l)
                    pair.append(padded(weight[tap].astype(F32), width))
                rows.append(padded(jnp.concatenate(pair, axis=1), LANES))
    tall = jnp.concatenate(rows, axis=0)
    target[...] = tall.T[: 2 * width].astype(BF16)


def shifted(block):
    wide = block.astype(F32)
    last = block.shape[1] - 1
    lane = lax.broadcasted_iota(jnp.int32, wide.shape, 1)
    low = jnp.where(lane == 0, 0.0, pltpu.roll(wide, 1, 1)).astype(BF16)
    high = jnp.where(lane == last, 0.0, pltpu.roll(wide, last, 1)).astype(BF16)
    return low, high


def fill(rows, y, z, first, block):
    height = block.shape[0]
    low, high = shifted(block)
    rows[y, z, 0, first : first + height, :] = low
    rows[y, z, 1, first : first + height, :] = block
    rows[y, z, 2, first : first + height, :] = high


def taken(rows, y):
    part = rows[pl.ds(y, 3)]
    return part.reshape(part.shape[0] * part.shape[1] * part.shape[2] * part.shape[3], part.shape[4])


def parted(wide, first, count):
    blocks = [wide[k, pl.ds(first, count, stride=2), :] for k in range(wide.shape[0])]
    return jnp.concatenate(blocks, axis=1).astype(BF16)


def merged(wide, first, block):
    for k in range(wide.shape[0]):
        wide[k, pl.ds(first, block.shape[0], stride=2), :] = block[
            :, k * LANES : (k + 1) * LANES
        ].astype(F32)


def rows_from(wide):
    return jnp.concatenate([wide[k] for k in range(wide.shape[0])], axis=1)


def weight_sum(rows, first, cots):
    total = None
    for r, cot in enumerate(cots):
        high, low = cot[32:64], cot[0:32]
        none = jnp.zeros_like(low)
        for zi in range(2):
            spread = [high, low, none, none] if zi == 0 else [none, high, low, none]
            part = rows[first + r : first + r + 3, zi]
            part = part.reshape(part.shape[0] * part.shape[1] * part.shape[2], part.shape[3])
            term = dot_nt(part, jnp.concatenate(spread, axis=0))
            total = term if total is None else total + term
    return total


def kernel(
    n,
    energy,
    volume,
    dual_state,
    sinogram,
    cot_volume,
    cot_dual,
    basis,
    footprint_table,
    tiles,
    kinds,
    places,
    counts,
    wpi,
    wpo,
    wdi,
    wdo,
    bpi,
    bpo,
    bdi,
    bdo,
    nv_out,
    nd_out,
    vg_out,
    dg_out,
    gp,
    gd,
    nv,
    nd,
    vg,
    dg,
    raw_vol,
    raw_cvol,
    raw_ds,
    raw_cd,
    raw_sino,
    table,
    wide,
    vol,
    cvol,
    ds,
    cd,
    sino,
    tw,
    pc,
    fpi,
    fpo,
    fdi,
    fdo,
    api,
    apo,
    adi,
    ado,
    s_d,
    s_dh,
    s_p,
    s_ph,
    s_c,
    s_pg,
    s_dc,
    s_dpg,
    ds_h,
    si_h,
    pr_h,
    vol_h,
    cvol_h,
    cd_h,
    bp_h,
    dc_h,
    pr_own,
    bp_own,
    dc_own,
    dpre,
    ppre,
    hgrad,
    ingrad,
    dtotal,
    dhg,
    rsum,
    pack,
    outbox,
    inbox,
    px_out,
    px_in,
    rs_out,
    rs_in,
    ag_own,
    ag_in,
    load,
    send,
    recv,
    hsend,
    hrecv,
):
    me = lax.axis_index(AXIS)
    chips = n // 2
    chip = me // 2
    core = me % 2
    partner = me + 1 - 2 * core
    channels = ds.shape[0] // 2
    width = ds.shape[1]
    columns = width // UW
    tables = table.shape[0]
    chunk = ag_own.shape[1]

    def to(offset):
        return lax.rem(me + offset + n, n)

    def far_first(k, count):
        half = lax.shift_right_logical(k, 1)
        return jnp.where(lax.bitwise_and(k, 1) == 0, count // 2 + half, count // 2 - 1 - half)

    def wrapped(index, count):
        return jnp.where(index >= count, index - count, index)

    def steps(low, high):
        return pl.loop(low, high, unroll=7 if (high - low) % 7 == 0 else 1)

    barrier = pltpu.get_barrier_semaphore()

    @steps(0, n - 1)
    def _(k):
        peer = wrapped(me + far_first(k, n), n)
        pl.semaphore_signal(barrier, inc=1, device_id={AXIS: peer}, device_id_type=MESH)

    loads = [
        pltpu.make_async_copy(source, target, load.at[i])
        for i, (source, target) in enumerate(
            (
                (volume, raw_vol),
                (footprint_table, table),
                (dual_state, raw_ds),
                (sinogram, raw_sino),
                (cot_volume, raw_cvol),
                (cot_dual, raw_cd),
            )
        )
    ]
    for copy in loads:
        copy.start()
    stores = [
        pltpu.make_async_copy(source, target, load.at[len(loads) + i])
        for i, (source, target) in enumerate(
            ((nv, nv_out), (nd, nd_out), (vg, vg_out), (dg, dg_out))
        )
    ]

    def exchange(source, target, phase, low=0, high=n - 1):
        @steps(low, high)
        def _(k):
            peer = wrapped(me + far_first(k, n), n)
            pltpu.make_async_remote_copy(
                src_ref=source.at[peer],
                dst_ref=target.at[me],
                send_sem=send.at[phase],
                recv_sem=recv.at[phase],
                device_id={AXIS: peer},
                device_id_type=MESH,
            ).start()

        if low == 0:
            target[me] = source[me]

    apart = 4
    members = chips // apart

    def slot_of(there):
        return (there % apart) * members + there // apart

    own_slot = slot_of(chip)

    def lanes(source, target, phase, same):
        @steps(0, chips - 1)
        def _(k):
            there = wrapped(chip + far_first(k, chips), chips)
            pltpu.make_async_remote_copy(
                src_ref=source if same else source.at[slot_of(there)],
                dst_ref=target.at[own_slot],
                send_sem=send.at[phase],
                recv_sem=recv.at[phase],
                device_id={AXIS: 2 * there + core},
                device_id_type=MESH,
            ).start()

        target[own_slot] = source[...] if same else source[own_slot]

    def class_far(source, target, phase):
        @steps(0, members - 1)
        def _(k):
            there = wrapped(chip + apart * far_first(k, members), chips)
            pltpu.make_async_remote_copy(
                src_ref=source,
                dst_ref=target.at[own_slot],
                send_sem=send.at[phase],
                recv_sem=recv.at[phase],
                device_id={AXIS: 2 * there + core},
                device_id_type=MESH,
            ).start()

        target[own_slot] = source[...]

    def class_near(target, phase):
        own = target.at[pl.ds((chip % apart) * members, members)]
        for step in (2, 1, chips - 1):
            pltpu.make_async_remote_copy(
                src_ref=own,
                dst_ref=own,
                send_sem=send.at[phase],
                recv_sem=recv.at[phase],
                device_id={AXIS: 2 * wrapped(chip + step, chips) + core},
                device_id_type=MESH,
            ).start()

    def all_of(target, phase, count=None):
        part = target.at[pl.ds(0, count or target.shape[0] - 1)]
        return pltpu.make_async_remote_copy(
            src_ref=part,
            dst_ref=part,
            send_sem=send.at[phase],
            recv_sem=recv.at[phase],
            device_id={AXIS: to(1)},
            device_id_type=MESH,
        )

    halos = []

    def halo(source, target, offsets, base):
        copies = []
        for slot, offset in enumerate(offsets):
            there = len(offsets) - 1 - slot
            copies.append(
                pltpu.make_async_remote_copy(
                    src_ref=source,
                    dst_ref=target.at[there],
                    send_sem=hsend.at[base + there],
                    recv_sem=hrecv.at[base + there],
                    device_id={AXIS: to(offset)},
                    device_id_type=MESH,
                )
            )
        for copy in copies:
            copy.start()
        halos.extend(copies)
        return copies

    def swap(source, target, phase):
        copy = pltpu.make_async_remote_copy(
            src_ref=source,
            dst_ref=target,
            send_sem=send.at[phase],
            recv_sem=recv.at[phase],
            device_id={AXIS: partner},
            device_id_type=MESH,
        )
        copy.start()
        halos.append(copy)
        return copy

    def footprints(q):
        return [dot(q, table[o]) for o in range(tables)]

    def spread(values, scale, target):
        @pl.loop(0, n, unroll=4)
        def _(b):
            total = scale[0, pl.ds(b, 1), :] * values[0]
            for o in range(1, len(values)):
                total = total + scale[o, pl.ds(b, 1), :] * values[o]
            target[b] = total.astype(BF16)

    def gathered(source, scale, count):
        def step(t, totals):
            block = source[t].astype(F32)
            return tuple(totals[c] + scale[c, pl.ds(t, 1), :] * block for c in range(count))

        start = tuple(jnp.zeros(source.shape[1:], F32) for _ in range(count))
        return lax.fori_loop(0, n, step, start, unroll=4)

    def q_of(y0, y1):
        return jnp.concatenate([y0, y1], axis=1)

    def tile_sums(groups):
        total = None
        for o in range(tables):
            high = groups[o].astype(BF16)
            low = (groups[o] - high.astype(F32)).astype(BF16)
            term = dot_nt(jnp.concatenate([high, low], axis=0), table[o])
            total = term if total is None else total + term
        return total[0:8] + total[8:16]

    entries = tiles.shape[0]
    entry = lax.broadcasted_iota(jnp.int32, (entries, n), 0)
    lane = lax.broadcasted_iota(jnp.int32, (entries, n), 1)
    ones = jnp.ones((entries, LANES), BF16)

    def flags(mask):
        return dot_tn(jnp.where(mask, 1.0, 0.0).astype(BF16), ones)

    tile, kind, place = tiles[...], kinds[...], places[...]
    live = entry < counts[...]
    for o in range(tables):
        tw[o] = flags(live & (tile == me) & (kind == o))

    def own_column(values):
        return jnp.sum(jnp.where(lane == me, values, 0.0), axis=1, keepdims=True)

    own_live = own_column(jnp.where(live, 1.0, 0.0))
    own_tile = own_column(tile.astype(F32))
    own_place = own_column(place.astype(F32))
    hit = (own_tile == lane.astype(F32)) & (own_live > 0.5)
    for c in range(columns):
        pc[c] = flags(hit & (own_place == float(c)))

    row = lax.broadcasted_iota(jnp.int32, (8, 8), 0)
    col = lax.broadcasted_iota(jnp.int32, (8, 8), 1)
    chosen = jnp.zeros((8, 8), F32)
    for b in range(4):
        chosen = chosen + jnp.where((row % 4 == b) & (col == energy[b]), 1.0, 0.0)
    mixing = dot(chosen.astype(BF16), basis[...])
    both_z = jnp.concatenate([mixing, mixing], axis=1)
    row = lax.broadcasted_iota(jnp.int32, both_z.shape, 0)
    col = lax.broadcasted_iota(jnp.int32, both_z.shape, 1)
    mix_wide = jnp.where(row // 4 == col // channels, both_z, 0.0)
    mix = mix_wide.astype(BF16)
    mix_twice = jnp.concatenate([mix_wide, mix_wide], axis=0).astype(BF16)

    def column_of(bias):
        row = lax.broadcasted_iota(jnp.int32, (2 * channels, channels), 0)
        col = lax.broadcasted_iota(jnp.int32, (2 * channels, channels), 1)
        return jnp.sum(jnp.where(row % channels == col, bias[...], 0.0), axis=1, keepdims=True)

    def slab(source, target):
        for z in range(2):
            part = source[:, z].astype(F32).reshape(2 * channels, width)
            for k in range(width // LANES):
                wide[k] = part[:, k * LANES : (k + 1) * LANES]
            for y in range(2):
                target[y, z * channels : (z + 1) * channels, :] = parted(wide, y, channels)

    def view_slab(source, target):
        count = source.shape[0]
        part = source[...].astype(F32).reshape(2 * count, width)
        for k in range(width // LANES):
            wide[k, 0 : 2 * count, :] = part[:, k * LANES : (k + 1) * LANES]
        if count % 16 == 0:
            for z in range(2):
                target[z * count : (z + 1) * count, :] = parted(wide, z, count)
        else:
            target[...] = jnp.concatenate(
                [parted(wide, z, count).astype(F32) for z in range(2)], axis=0
            ).astype(BF16)

    loads[0].wait()
    slab(raw_vol, vol)
    loads[1].wait()
    bins = q_of(dot(mix, vol[0]), dot(mix, vol[1])).astype(BF16)
    spread(footprints(bins), tw, outbox.at[0])
    loads[2].wait()
    view_slab(raw_ds, ds)
    loads[3].wait()
    view_slab(raw_sino, sino)
    loads[4].wait()
    slab(raw_cvol, cvol)
    loads[5].wait()
    view_slab(raw_cd, cd)
    forward_weights(wdi, fdi, 48)
    forward_weights(wdo, fdo, 32)
    forward_weights(wpi, fpi, 48)
    forward_weights(wpo, fpo, 32)
    adjoint_weights(wpo, apo, 32)
    adjoint_weights(wpi, api, 48)
    adjoint_weights(wdo, ado, 32)
    adjoint_weights(wdi, adi, 48)
    pl.semaphore_wait(barrier, n - 1)
    exchange(outbox.at[0], inbox.at[0], 0)
    ds_copies = halo(ds, ds_h, OFFS, 0)
    si_copies = halo(sino, si_h, OFFS, 4)
    def fill_views(rows, own, others, first):
        for z in range(2):
            fill(rows, 2, z, first, own[z * channels : (z + 1) * channels, :])
        for slot, view in enumerate((0, 1, 3, 4)):
            for z in range(2):
                fill(rows, view, z, first, others[slot, z * channels : (z + 1) * channels, :])

    for copy in ds_copies:
        copy.wait_recv()
    fill_views(s_d, ds, ds_h, 0)
    for copy in si_copies:
        copy.wait_recv()

    all_of(inbox.at[0], 0).wait_recv()
    windows = gathered(inbox.at[0], pc, columns)
    pr_own[...] = jnp.concatenate(windows, axis=1).astype(BF16)
    pr_copies = halo(pr_own, pr_h, OFFS, 8)
    vol_copies = halo(vol, vol_h, (-1, 1), 12)
    cvol_copies = halo(cvol, cvol_h, (-1, 1), 14)

    def fill_tail(view, projected, measured):
        for z in range(2):
            block = jnp.concatenate(
                [
                    projected[z * 4 : z * 4 + 4].astype(F32),
                    measured[z * 4 : z * 4 + 4].astype(F32),
                    jnp.zeros((8, width), F32),
                ],
                axis=0,
            ).astype(BF16)
            fill(s_d, view, z, channels, block)

    fill_tail(2, pr_own[...], sino[...])
    for copy in pr_copies:
        copy.wait_recv()
    for slot, view in enumerate((0, 1, 3, 4)):
        fill_tail(view, pr_h[slot], si_h[slot])

    bias_di = column_of(bdi)

    @pl.loop(0, 3)
    def _(v):
        pre = dot(fdi[...], taken(s_d, v)) + bias_di
        dpre[v] = pre
        hidden = (pre * sigmoid(pre)).astype(BF16)
        for z in range(2):
            fill(s_dh, v, z, 0, hidden[z * channels : (z + 1) * channels])

    update = dot(fdo[...], taken(s_dh, 0)) + column_of(bdo)
    fresh = (ds[...].astype(F32) + update).astype(BF16)
    nd[...] = fresh
    stores[1].start()

    def bins_of(block, stride, first):
        return jnp.concatenate(
            [block[first : first + 4], block[stride + first : stride + first + 4]], axis=0
        )

    def parts_of(signal):
        return [signal[:, c * UW : (c + 1) * UW] for c in range(columns)]

    spread(parts_of(bins_of(fresh.astype(F32), channels, 0)), pc, outbox.at[1])
    exchange(outbox.at[1], inbox.at[1], 1)
    cd_copies = halo(cd, cd_h, OFFS, 16)

    low_in = jnp.where(me > 0, 1.0, 0.0).astype(F32)
    high_in = jnp.where(me < n - 1, 1.0, 0.0).astype(F32)

    def fill_rows(rows, own, others):
        for y in range(2):
            for z in range(2):
                part = slice(z * channels, (z + 1) * channels)
                fill(rows, 2 + y, z, 0, own[y, part, :])
                fill(rows, y, z, 0, (others[0, y, part, :].astype(F32) * low_in).astype(BF16))
                fill(rows, 4 + y, z, 0, (others[1, y, part, :].astype(F32) * high_in).astype(BF16))

    for copy in cvol_copies:
        copy.wait_recv()
    fill_rows(s_c, cvol, cvol_h)

    @pl.loop(0, 4)
    def _(r):
        hgrad[r] = dot(apo[...], taken(s_c, r))

    for copy in vol_copies:
        copy.wait_recv()
    fill_rows(s_p, vol, vol_h)

    all_of(inbox.at[1], 1).wait_recv()
    summed = tile_sums(gathered(inbox.at[1], tw, tables))
    bp_own[...] = summed.astype(BF16)
    bp_copies = halo(bp_own, bp_h, (-1, 1), 20)

    def fill_back(row, block):
        for z in range(2):
            part = jnp.concatenate(
                [block[z * 4 : z * 4 + 4], jnp.zeros((12, width), F32)], axis=0
            ).astype(BF16)
            fill(s_p, row, z, channels, part)

    own_back = bp_own[...].astype(F32)
    for y in range(2):
        fill_back(2 + y, own_back[:, y * width : (y + 1) * width])
    for copy in bp_copies:
        copy.wait_recv()
    low_back = bp_h[0].astype(F32) * low_in
    high_back = bp_h[1].astype(F32) * high_in
    for y in range(2):
        fill_back(y, low_back[:, y * width : (y + 1) * width])
        fill_back(4 + y, high_back[:, y * width : (y + 1) * width])

    bias_pi = column_of(bpi)

    @pl.loop(0, 4)
    def _(r):
        pre = dot(fpi[...], taken(s_p, r)) + bias_pi
        ppre[r] = pre
        inside = jnp.where(r == 0, low_in, jnp.where(r == 3, high_in, 1.0))
        s = sigmoid(pre)
        grad = (hgrad[r] * (s * (1.0 + pre * (1.0 - s))) * inside).astype(BF16)
        for z in range(2):
            fill(s_pg, r, z, 0, grad[z * channels : (z + 1) * channels])

    for r in range(2):
        ingrad[r] = dot(api[...], taken(s_pg, r))
    back = q_of(bins_of(ingrad[0], 48, channels), bins_of(ingrad[1], 48, channels)).astype(BF16)
    spread(footprints(back), tw, outbox.at[2])
    exchange(outbox.at[2], inbox.at[2], 2)

    @pl.loop(0, 4)
    def _(r):
        pre = ppre[r]
        inside = jnp.where(r == 0, low_in, jnp.where(r == 3, high_in, 1.0))
        hidden = (pre * sigmoid(pre) * inside).astype(BF16)
        for z in range(2):
            fill(s_ph, r, z, 0, hidden[z * channels : (z + 1) * channels])

    def packed(inner, outer, side):
        for k in range(9):
            rsum[k * 40 : (k + 1) * 40, :] = inner[k * 48 : k * 48 + 40]
        rsum[360:648, :] = outer
        lane = lax.broadcasted_iota(jnp.int32, (160, LANES), 1)
        tail = rsum[488:648, :]
        for i in range(3):
            moved = tail if i == 3 else pltpu.roll(tail, 96 - 32 * i, 1)
            pack[i * 160 : (i + 1) * 160, :] = jnp.where(
                lane < 96, rsum[i * 160 : (i + 1) * 160, :], moved
            )
        pack[480:488, :] = rsum[480:488, :]
        pack[488:512, :] = jnp.zeros((24, LANES), F32)
        px_out[side] = pack[pl.ds(other_half, 256), :].reshape(chips, chunk, LANES)
        return swap(px_out.at[side], px_in.at[side], 8 + side)

    own_half = pl.multiple_of(core * 256, 256)
    other_half = pl.multiple_of(256 - core * 256, 256)

    def chip_sum(side, copy):
        copy.wait_recv()
        own = pack[pl.ds(own_half, 256), :].reshape(chips, chunk, LANES)
        rs_out[side] = (own + px_in[side]).astype(BF16)

    def own_rows(rows, y):
        return jnp.concatenate([rows[y, 0, 1], rows[y, 1, 1]], axis=0)

    half_p = packed(
        weight_sum(s_p, 1, [own_rows(s_pg, 1), own_rows(s_pg, 2)]),
        weight_sum(s_ph, 0, [cvol[0], cvol[1]]),
        0,
    )
    for r in range(2):
        change = dot(fpo[...], taken(s_ph, r)) + column_of(bpo)
        nv[r] = (vol[r].astype(F32) + change).astype(BF16)
    stores[0].start()

    chip_sum(0, half_p)
    for copy in cd_copies:
        copy.wait_recv()

    def reduced(side):
        all_of(rs_in.at[side], 4 + side).wait_recv()

        def step(t, total):
            return total + rs_in[side, t].astype(F32)

        total = lax.fori_loop(0, chips, step, jnp.zeros((chunk, LANES), F32), unroll=4)
        ag_own[side] = total.astype(BF16)

    all_of(inbox.at[2], 2).wait_recv()
    toward = jnp.concatenate(gathered(inbox.at[2], pc, columns), axis=1)
    own_cot = cd[...].astype(F32)
    dtotal[...] = own_cot
    dtotal[0:4, :] = own_cot[0:4] + toward[0:4]
    dtotal[channels : channels + 4, :] = own_cot[channels : channels + 4] + toward[4:8]
    dc_own[...] = bins_of(dtotal[...], channels, 0).astype(BF16)
    dc_copies = halo(dc_own, dc_h, OFFS, 22)
    lanes(rs_out.at[0], rs_in.at[0], 4, False)
    own_total = dtotal[...].astype(BF16)
    for z in range(2):
        fill(s_dc, 2, z, 0, own_total[z * channels : (z + 1) * channels])
    for copy in dc_copies:
        copy.wait_recv()
    for slot, view in enumerate((0, 1, 3, 4)):
        for z in range(2):
            block = jnp.concatenate(
                [
                    dc_h[slot, z * 4 : z * 4 + 4, :].astype(F32),
                    cd_h[slot, z * channels + 4 : (z + 1) * channels, :].astype(F32),
                ],
                axis=0,
            ).astype(BF16)
            fill(s_dc, view, z, 0, block)

    @pl.loop(0, 3)
    def _(v):
        pre = dpre[v]
        s = sigmoid(pre)
        grad = (dot(ado[...], taken(s_dc, v)) * (s * (1.0 + pre * (1.0 - s)))).astype(BF16)
        for z in range(2):
            fill(s_dpg, v, z, 0, grad[z * channels : (z + 1) * channels])

    half_d = packed(
        weight_sum(s_d, 1, [own_rows(s_dpg, 1)]),
        weight_sum(s_dh, 0, [own_total]),
        1,
    )
    dhg[...] = dot(adi[...], taken(s_dpg, 0))
    spread(parts_of(bins_of(dhg[...], 48, channels).astype(BF16).astype(F32)), pc, outbox.at[3])
    chip_sum(1, half_d)
    lanes(rs_out.at[1], rs_in.at[1], 5, False)
    cut = 7 * ((n - 1) // 14)
    exchange(outbox.at[3], inbox.at[3], 3, 0, cut)
    for z in range(2):
        part = slice(z * channels, (z + 1) * channels)
        dg[part, :] = (dtotal[part, :] + dhg[z * 48 : z * 48 + channels, :]).astype(BF16)
    stores[3].start()
    reduced(0)
    class_far(ag_own.at[0], ag_in.at[0, core], 6)
    reduced(1)
    lanes(ag_own.at[1], ag_in.at[1, core], 7, True)
    exchange(outbox.at[3], inbox.at[3], 3, cut, n - 1)
    all_of(ag_in.at[0, core], 6, members - 1).wait_recv()
    class_near(ag_in.at[0, core], 12)
    all_of(ag_in.at[0, core], 12, 3 * members).wait_recv()
    swaps = [swap(ag_in.at[0, core], ag_in.at[0, core], 10)]
    all_of(ag_in.at[1, core], 7).wait_recv()
    swaps.append(swap(ag_in.at[1, core], ag_in.at[1, core], 11))

    all_of(inbox.at[3], 3).wait_recv()
    final = tile_sums(gathered(inbox.at[3], tw, tables))
    high = final.astype(BF16)
    low = (final - high.astype(F32)).astype(BF16)
    both = jnp.concatenate([high.astype(F32), low.astype(F32)], axis=0).astype(BF16)
    for y in range(2):
        mixed = dot_tn(mix_twice, both[:, y * width : (y + 1) * width])
        for z in range(2):
            part = slice(z * channels, (z + 1) * channels)
            vg[y, part, :] = (
                cvol[y, part, :].astype(F32)
                + ingrad[y, z * 48 : z * 48 + channels, :]
                + mixed[part]
            ).astype(BF16)
    stores[2].start()

    for side, result in enumerate((gp, gd)):
        swaps[side].wait_recv()
        result[...] = ag_in[side].reshape(result.shape)

    for phase in range(4):
        all_of(inbox.at[phase], phase).wait_send()
    for side in range(2):
        all_of(rs_in.at[side], 4 + side).wait_send()
    all_of(ag_in.at[0, core], 6, members - 1).wait_send()
    all_of(ag_in.at[0, core], 12, 3 * members).wait_send()
    all_of(ag_in.at[1, core], 7).wait_send()
    for copy in halos:
        copy.wait_send()
    for copy in stores:
        copy.wait()


def finish(*refs):
    sources, targets, held, made = refs[:6], refs[6:14], refs[14:20], refs[20:28]
    wide, tall, load, store = refs[28:]
    loads = [pltpu.make_async_copy(a, b, load.at[i]) for i, (a, b) in enumerate(zip(sources, held))]
    stores = [pltpu.make_async_copy(a, b, store.at[i]) for i, (a, b) in enumerate(zip(made, targets))]
    for i in (4, 5, 0, 2, 1, 3):
        loads[i].start()
    channels = made[1].shape[0]
    width = made[1].shape[2]

    for side in range(2):
        loads[4 + side].wait()
        packed = held[4 + side]
        tall[0:488, :] = packed[0:488, :].astype(F32)
        lane = lax.broadcasted_iota(jnp.int32, (160, LANES), 1)
        rows = jnp.zeros((160, LANES), F32)
        for i in range(3):
            block = packed[i * 160 : (i + 1) * 160, :].astype(F32)
            rows = jnp.where(lane // 32 == i, pltpu.roll(block, 32 * (i + 1), 1), rows)
        tall[488:648, :] = rows
        tall[648:, :] = jnp.zeros((tall.shape[0] - 648, LANES), F32)
        flat = tall[...].T
        inner, outer = made[4 + 2 * side], made[5 + 2 * side]
        for i in range(3):
            part = flat[i * 32 : (i + 1) * 32]
            for k in range(9):
                inner[9 * i + k] = part[:, k * 40 : k * 40 + inner.shape[2]]
                outer[9 * i + k] = part[:, 360 + k * 32 : 360 + k * 32 + outer.shape[2]]
        stores[4 + 2 * side].start()
        stores[5 + 2 * side].start()

    for which in (0, 2):
        loads[which].wait()
        for z in range(2):
            for y in range(2):
                merged(wide, y, held[which][y, z * channels : (z + 1) * channels, :])
            made[which][:, z] = rows_from(wide).reshape(channels, 2, width).astype(BF16)
        stores[which].start()
    for which in (1, 3):
        loads[which].wait()
        for z in range(2):
            merged(wide, z, held[which][z * channels : (z + 1) * channels, :])
        made[which][...] = rows_from(wide).reshape(channels, 2, width).astype(BF16)
        stores[which].start()
    for copy in stores:
        copy.wait()


def shards(
    n,
    volume,
    dual_state,
    sinogram,
    cot_volume,
    cot_dual,
    basis_table,
    bin_energy,
    footprint_table,
    hit_tile,
    hit_table,
    hit_column,
    hit_count,
    primal_inner,
    primal_inner_bias,
    primal_outer,
    primal_outer_bias,
    dual_inner,
    dual_inner_bias,
    dual_outer,
    dual_outer_bias,
):
    channels, slices, row_count, width = volume.shape
    bin_count = sinogram.shape[0]
    columns = width // UW
    tables = footprint_table.shape[0]
    both = slices * channels

    chunk = 512 // n
    vmem = pl.BlockSpec(memory_space=pltpu.VMEM)
    smem = pl.BlockSpec(memory_space=pltpu.SMEM)
    shape = jax.ShapeDtypeStruct

    def rows_of(y, c):
        return pltpu.VMEM((y, 2, 3, c, width), BF16)

    any_space = pl.BlockSpec(memory_space=pl.ANY)
    messages = (n, slices * bin_count, UW)
    new_volume, new_dual, volume_grad, dual_grad, packed_primal, packed_dual = pl.pallas_call(
        functools.partial(kernel, n),
        out_shape=(
            shape((row_count, both, width), BF16),
            shape((both, width), BF16),
            shape((row_count, both, width), BF16),
            shape((both, width), BF16),
            shape((n * chunk, LANES), BF16),
            shape((n * chunk, LANES), BF16),
        ),
        in_specs=[smem] + [any_space] * 5 + [vmem, any_space] + [vmem] * 12,
        out_specs=(any_space,) * 4 + (vmem,) * 2,
        scratch_shapes=[
            pltpu.VMEM((row_count, both, width), BF16),
            pltpu.VMEM((both, width), BF16),
            pltpu.VMEM((row_count, both, width), BF16),
            pltpu.VMEM((both, width), BF16),
            pltpu.VMEM(volume.shape, BF16),
            pltpu.VMEM(volume.shape, BF16),
            pltpu.VMEM((channels, slices, width), BF16),
            pltpu.VMEM((channels, slices, width), BF16),
            pltpu.VMEM((bin_count, slices, width), BF16),
            pltpu.VMEM(footprint_table.shape, BF16),
            pltpu.VMEM((width // LANES, both, LANES), F32),
            pltpu.VMEM((row_count, both, width), BF16),
            pltpu.VMEM((row_count, both, width), BF16),
            pltpu.VMEM((both, width), BF16),
            pltpu.VMEM((both, width), BF16),
            pltpu.VMEM((slices * bin_count, width), BF16),
            pltpu.VMEM((tables, n, LANES), F32),
            pltpu.VMEM((columns, n, LANES), F32),
            pltpu.VMEM((64, 18 * 48), BF16),
            pltpu.VMEM((64, 18 * 32), BF16),
            pltpu.VMEM((64, 18 * 48), BF16),
            pltpu.VMEM((64, 18 * 32), BF16),
            pltpu.VMEM((96, 18 * 32), BF16),
            pltpu.VMEM((64, 18 * 32), BF16),
            pltpu.VMEM((96, 18 * 32), BF16),
            pltpu.VMEM((64, 18 * 32), BF16),
            rows_of(5, 48),
            rows_of(3, 32),
            rows_of(6, 48),
            rows_of(4, 32),
            rows_of(6, 32),
            rows_of(4, 32),
            rows_of(5, 32),
            rows_of(3, 32),
            pltpu.VMEM((4, both, width), BF16),
            pltpu.VMEM((4, 8, width), BF16),
            pltpu.VMEM((4, 8, width), BF16),
            pltpu.VMEM((2, row_count, both, width), BF16),
            pltpu.VMEM((2, row_count, both, width), BF16),
            pltpu.VMEM((4, both, width), BF16),
            pltpu.VMEM((2, 8, row_count * width), BF16),
            pltpu.VMEM((4, 8, width), BF16),
            pltpu.VMEM((8, width), BF16),
            pltpu.VMEM((8, row_count * width), BF16),
            pltpu.VMEM((8, width), BF16),
            pltpu.VMEM((3, both, width), F32),
            pltpu.VMEM((4, both, width), F32),
            pltpu.VMEM((4, both, width), F32),
            pltpu.VMEM((2, 96, width), F32),
            pltpu.VMEM((both, width), F32),
            pltpu.VMEM((96, width), F32),
            pltpu.VMEM((648, LANES), F32),
            pltpu.VMEM((512, LANES), F32),
            pltpu.VMEM((4,) + messages, BF16),
            pltpu.VMEM((4,) + messages, BF16),
            pltpu.VMEM((2, n // 2, chunk, LANES), F32),
            pltpu.VMEM((2, n // 2, chunk, LANES), F32),
            pltpu.VMEM((2, n // 2, chunk, LANES), BF16),
            pltpu.VMEM((2, n // 2, chunk, LANES), BF16),
            pltpu.VMEM((2, chunk, LANES), BF16),
            pltpu.VMEM((2, 2, n // 2, chunk, LANES), BF16),
            pltpu.SemaphoreType.DMA((10,)),
            pltpu.SemaphoreType.DMA((13,)),
            pltpu.SemaphoreType.DMA((13,)),
            pltpu.SemaphoreType.DMA((26,)),
            pltpu.SemaphoreType.DMA((26,)),
        ],
        compiler_params=pltpu.CompilerParams(
            collective_id=0, has_side_effects=True, vmem_limit_bytes=60 * 1024 * 1024
        ),
    )(
        bin_energy,
        volume,
        dual_state.reshape(channels, slices, width),
        sinogram.reshape(bin_count, slices, width),
        cot_volume,
        cot_dual.reshape(channels, slices, width),
        basis_table,
        footprint_table,
        hit_tile.T,
        hit_table.T,
        hit_column.T,
        hit_count.reshape(1, n),
        primal_inner,
        primal_outer,
        dual_inner,
        dual_outer,
        *(
            b.reshape(1, channels)
            for b in (primal_inner_bias, primal_outer_bias, dual_inner_bias, dual_outer_bias)
        ),
    )
    halves = (new_volume, new_dual, volume_grad, dual_grad, packed_primal, packed_dual)
    finals = (
        shape(volume.shape, BF16),
        shape((channels, slices, width), BF16),
        shape(volume.shape, BF16),
        shape((channels, slices, width), BF16),
        *(shape(w.shape, F32) for w in (primal_inner, primal_outer, dual_inner, dual_outer)),
    )
    new_volume, new_dual, volume_grad, dual_grad, *gradients = pl.pallas_call(
        finish,
        out_shape=finals,
        in_specs=[any_space] * 6,
        out_specs=(any_space,) * 8,
        scratch_shapes=[
            *(pltpu.VMEM(a.shape, a.dtype) for a in halves),
            *(pltpu.VMEM(a.shape, a.dtype) for a in finals),
            pltpu.VMEM((width // LANES, both, LANES), F32),
            pltpu.VMEM((768, LANES), F32),
            pltpu.SemaphoreType.DMA((6,)),
            pltpu.SemaphoreType.DMA((8,)),
        ],
    )(*halves)
    return (
        new_volume,
        new_dual.reshape(dual_state.shape),
        volume_grad,
        dual_grad.reshape(dual_state.shape),
        *gradients,
    )


def solution(mesh):
    part = P(None, "parts", AXIS, None)
    return jax.shard_map(
        functools.partial(shards, mesh.shape[AXIS]),
        mesh=mesh,
        in_specs=(part,) * 5 + (P(),) * 15,
        out_specs=(part,) * 4 + (P("parts", None, None),) * 4,
        check_vma=False,
    )
```

```python
import functools

import jax
import jax.numpy as jnp
from jax import lax
from jax.experimental import pallas as pl
from jax.experimental.pallas import tpu as pltpu
from jax.sharding import PartitionSpec as P

F32 = jnp.float32
BF16 = jnp.bfloat16
MESH = pl.DeviceIdType.MESH
AXIS = "view"
UW = 128
LANES = 128
OFFS = (-2, -1, 1, 2)


def dot(a, b):
    return jnp.dot(a, b, preferred_element_type=F32)


def dot_tn(a, b):
    return lax.dot_general(a, b, (((0,), (0,)), ((), ())), preferred_element_type=F32)


def dot_nt(a, b):
    return lax.dot_general(a, b, (((1,), (1,)), ((), ())), preferred_element_type=F32)


def sigmoid(a):
    return 1.0 / (1.0 + jnp.exp(-a))


def padded(piece, width):
    if piece.shape[1] == width:
        return piece
    return jnp.concatenate(
        [piece, jnp.zeros((piece.shape[0], width - piece.shape[1]), piece.dtype)], axis=1
    )


def forward_weights(weight, target, width):
    outs = weight.shape[1]
    for zo in range(2):
        pieces = []
        for j in range(3):
            for zi in range(2):
                for l in range(3):
                    tap = 9 * (zi - zo + 1) + 3 * j + l
                    pieces.append(padded(weight[tap].astype(F32), width))
        target[zo * outs : (zo + 1) * outs, :] = jnp.concatenate(pieces, axis=1).astype(BF16)


def adjoint_weights(weight, target, width):
    rows = []
    for j in range(3):
        for zi in range(2):
            for l in range(3):
                pair = []
                for zo in range(2):
                    tap = 26 - (9 * (zi - zo + 1) + 3 * j + l)
                    pair.append(padded(weight[tap].astype(F32), width))
                rows.append(padded(jnp.concatenate(pair, axis=1), LANES))
    tall = jnp.concatenate(rows, axis=0)
    target[...] = tall.T[: 2 * width].astype(BF16)


def shifted(block):
    wide = block.astype(F32)
    last = block.shape[1] - 1
    lane = lax.broadcasted_iota(jnp.int32, wide.shape, 1)
    low = jnp.where(lane == 0, 0.0, pltpu.roll(wide, 1, 1)).astype(BF16)
    high = jnp.where(lane == last, 0.0, pltpu.roll(wide, last, 1)).astype(BF16)
    return low, high


def fill(rows, y, z, first, block):
    height = block.shape[0]
    low, high = shifted(block)
    rows[y, z, 0, first : first + height, :] = low
    rows[y, z, 1, first : first + height, :] = block
    rows[y, z, 2, first : first + height, :] = high


def taken(rows, y):
    part = rows[pl.ds(y, 3)]
    return part.reshape(part.shape[0] * part.shape[1] * part.shape[2] * part.shape[3], part.shape[4])


def parted(wide, first, count):
    blocks = [wide[k, pl.ds(first, count, stride=2), :] for k in range(wide.shape[0])]
    return jnp.concatenate(blocks, axis=1).astype(BF16)


def merged(wide, first, block):
    for k in range(wide.shape[0]):
        wide[k, pl.ds(first, block.shape[0], stride=2), :] = block[
            :, k * LANES : (k + 1) * LANES
        ].astype(F32)


def rows_from(wide):
    return jnp.concatenate([wide[k] for k in range(wide.shape[0])], axis=1)


def weight_sum(rows, first, cots):
    total = None
    for r, cot in enumerate(cots):
        high, low = cot[32:64], cot[0:32]
        none = jnp.zeros_like(low)
        for zi in range(2):
            spread = [high, low, none, none] if zi == 0 else [none, high, low, none]
            part = rows[first + r : first + r + 3, zi]
            part = part.reshape(part.shape[0] * part.shape[1] * part.shape[2], part.shape[3])
            term = dot_nt(part, jnp.concatenate(spread, axis=0))
            total = term if total is None else total + term
    return total


def kernel(
    n,
    energy,
    volume,
    dual_state,
    sinogram,
    cot_volume,
    cot_dual,
    basis,
    footprint_table,
    tiles,
    kinds,
    places,
    counts,
    wpi,
    wpo,
    wdi,
    wdo,
    bpi,
    bpo,
    bdi,
    bdo,
    nv_out,
    nd_out,
    vg_out,
    dg_out,
    gp,
    gd,
    nv,
    nd,
    vg,
    dg,
    raw_vol,
    raw_cvol,
    raw_ds,
    raw_cd,
    raw_sino,
    table,
    wide,
    vol,
    cvol,
    ds,
    cd,
    sino,
    tw,
    pc,
    fpi,
    fpo,
    fdi,
    fdo,
    api,
    apo,
    adi,
    ado,
    s_d,
    s_dh,
    s_p,
    s_ph,
    s_c,
    s_pg,
    s_dc,
    s_dpg,
    ds_h,
    si_h,
    pr_h,
    vol_h,
    cvol_h,
    cd_h,
    bp_h,
    dc_h,
    pr_own,
    bp_own,
    dc_own,
    dpre,
    ppre,
    hgrad,
    ingrad,
    dtotal,
    dhg,
    rsum,
    pack,
    outbox,
    inbox,
    px_out,
    px_in,
    rs_out,
    rs_in,
    ag_own,
    ag_in,
    load,
    send,
    recv,
    hsend,
    hrecv,
):
    me = lax.axis_index(AXIS)
    chips = n // 2
    chip = me // 2
    core = me % 2
    partner = me + 1 - 2 * core
    channels = ds.shape[0] // 2
    width = ds.shape[1]
    columns = width // UW
    tables = table.shape[0]
    chunk = ag_own.shape[1]

    def to(offset):
        return lax.rem(me + offset + n, n)

    def far_first(k, count):
        half = lax.shift_right_logical(k, 1)
        return jnp.where(lax.bitwise_and(k, 1) == 0, count // 2 + half, count // 2 - 1 - half)

    def wrapped(index, count):
        return jnp.where(index >= count, index - count, index)

    def steps(low, high):
        return pl.loop(low, high, unroll=7 if (high - low) % 7 == 0 else 1)

    barrier = pltpu.get_barrier_semaphore()

    @steps(0, n - 1)
    def _(k):
        peer = wrapped(me + far_first(k, n), n)
        pl.semaphore_signal(barrier, inc=1, device_id={AXIS: peer}, device_id_type=MESH)

    loads = [
        pltpu.make_async_copy(source, target, load.at[i])
        for i, (source, target) in enumerate(
            (
                (volume, raw_vol),
                (footprint_table, table),
                (dual_state, raw_ds),
                (sinogram, raw_sino),
                (cot_volume, raw_cvol),
                (cot_dual, raw_cd),
            )
        )
    ]
    for copy in loads:
        copy.start()
    stores = [
        pltpu.make_async_copy(source, target, load.at[len(loads) + i])
        for i, (source, target) in enumerate(
            ((nv, nv_out), (nd, nd_out), (vg, vg_out), (dg, dg_out))
        )
    ]

    def exchange(source, target, phase, low=0, high=n - 1):
        @steps(low, high)
        def _(k):
            peer = wrapped(me + far_first(k, n), n)
            pltpu.make_async_remote_copy(
                src_ref=source.at[peer],
                dst_ref=target.at[me],
                send_sem=send.at[phase],
                recv_sem=recv.at[phase],
                device_id={AXIS: peer},
                device_id_type=MESH,
            ).start()

        if low == 0:
            target[me] = source[me]

    apart = 4
    members = chips // apart

    def slot_of(there):
        return (there % apart) * members + there // apart

    own_slot = slot_of(chip)

    def lanes(source, target, phase, same):
        @steps(0, chips - 1)
        def _(k):
            there = wrapped(chip + far_first(k, chips), chips)
            pltpu.make_async_remote_copy(
                src_ref=source if same else source.at[slot_of(there)],
                dst_ref=target.at[own_slot],
                send_sem=send.at[phase],
                recv_sem=recv.at[phase],
                device_id={AXIS: 2 * there + core},
                device_id_type=MESH,
            ).start()

        target[own_slot] = source[...] if same else source[own_slot]

    def class_far(source, target, phase):
        @steps(0, members - 1)
        def _(k):
            there = wrapped(chip + apart * far_first(k, members), chips)
            pltpu.make_async_remote_copy(
                src_ref=source,
                dst_ref=target.at[own_slot],
                send_sem=send.at[phase],
                recv_sem=recv.at[phase],
                device_id={AXIS: 2 * there + core},
                device_id_type=MESH,
            ).start()

        target[own_slot] = source[...]

    def class_near(target, phase):
        own = target.at[pl.ds((chip % apart) * members, members)]
        for step in (2, 1, chips - 1):
            pltpu.make_async_remote_copy(
                src_ref=own,
                dst_ref=own,
                send_sem=send.at[phase],
                recv_sem=recv.at[phase],
                device_id={AXIS: 2 * wrapped(chip + step, chips) + core},
                device_id_type=MESH,
            ).start()

    def all_of(target, phase, count=None):
        part = target.at[pl.ds(0, count or target.shape[0] - 1)]
        return pltpu.make_async_remote_copy(
            src_ref=part,
            dst_ref=part,
            send_sem=send.at[phase],
            recv_sem=recv.at[phase],
            device_id={AXIS: to(1)},
            device_id_type=MESH,
        )

    halos = []

    def halo(source, target, offsets, base):
        copies = []
        for slot, offset in enumerate(offsets):
            there = len(offsets) - 1 - slot
            copies.append(
                pltpu.make_async_remote_copy(
                    src_ref=source,
                    dst_ref=target.at[there],
                    send_sem=hsend.at[base + there],
                    recv_sem=hrecv.at[base + there],
                    device_id={AXIS: to(offset)},
                    device_id_type=MESH,
                )
            )
        for copy in copies:
            copy.start()
        halos.extend(copies)
        return copies

    def swap(source, target, phase):
        copy = pltpu.make_async_remote_copy(
            src_ref=source,
            dst_ref=target,
            send_sem=send.at[phase],
            recv_sem=recv.at[phase],
            device_id={AXIS: partner},
            device_id_type=MESH,
        )
        copy.start()
        halos.append(copy)
        return copy

    def footprints(q):
        return [dot(q, table[o]) for o in range(tables)]

    def spread(values, scale, target):
        @pl.loop(0, n, unroll=4)
        def _(b):
            total = scale[0, pl.ds(b, 1), :] * values[0]
            for o in range(1, len(values)):
                total = total + scale[o, pl.ds(b, 1), :] * values[o]
            target[b] = total.astype(BF16)

    def gathered(source, scale, count):
        def step(t, totals):
            block = source[t].astype(F32)
            return tuple(totals[c] + scale[c, pl.ds(t, 1), :] * block for c in range(count))

        start = tuple(jnp.zeros(source.shape[1:], F32) for _ in range(count))
        return lax.fori_loop(0, n, step, start, unroll=4)

    def q_of(y0, y1):
        return jnp.concatenate([y0, y1], axis=1)

    def tile_sums(groups):
        total = None
        for o in range(tables):
            high = groups[o].astype(BF16)
            low = (groups[o] - high.astype(F32)).astype(BF16)
            term = dot_nt(jnp.concatenate([high, low], axis=0), table[o])
            total = term if total is None else total + term
        return total[0:8] + total[8:16]

    entries = tiles.shape[0]
    entry = lax.broadcasted_iota(jnp.int32, (entries, n), 0)
    lane = lax.broadcasted_iota(jnp.int32, (entries, n), 1)
    ones = jnp.ones((entries, LANES), BF16)

    def flags(mask):
        return dot_tn(jnp.where(mask, 1.0, 0.0).astype(BF16), ones)

    tile, kind, place = tiles[...], kinds[...], places[...]
    live = entry < counts[...]
    for o in range(tables):
        tw[o] = flags(live & (tile == me) & (kind == o))

    def own_column(values):
        return jnp.sum(jnp.where(lane == me, values, 0.0), axis=1, keepdims=True)

    own_live = own_column(jnp.where(live, 1.0, 0.0))
    own_tile = own_column(tile.astype(F32))
    own_place = own_column(place.astype(F32))
    hit = (own_tile == lane.astype(F32)) & (own_live > 0.5)
    for c in range(columns):
        pc[c] = flags(hit & (own_place == float(c)))

    row = lax.broadcasted_iota(jnp.int32, (8, 8), 0)
    col = lax.broadcasted_iota(jnp.int32, (8, 8), 1)
    chosen = jnp.zeros((8, 8), F32)
    for b in range(4):
        chosen = chosen + jnp.where((row % 4 == b) & (col == energy[b]), 1.0, 0.0)
    mixing = dot(chosen.astype(BF16), basis[...])
    both_z = jnp.concatenate([mixing, mixing], axis=1)
    row = lax.broadcasted_iota(jnp.int32, both_z.shape, 0)
    col = lax.broadcasted_iota(jnp.int32, both_z.shape, 1)
    mix_wide = jnp.where(row // 4 == col // channels, both_z, 0.0)
    mix = mix_wide.astype(BF16)
    mix_twice = jnp.concatenate([mix_wide, mix_wide], axis=0).astype(BF16)

    def column_of(bias):
        row = lax.broadcasted_iota(jnp.int32, (2 * channels, channels), 0)
        col = lax.broadcasted_iota(jnp.int32, (2 * channels, channels), 1)
        return jnp.sum(jnp.where(row % channels == col, bias[...], 0.0), axis=1, keepdims=True)

    def slab(source, target):
        for z in range(2):
            part = source[:, z].astype(F32).reshape(2 * channels, width)
            for k in range(width // LANES):
                wide[k] = part[:, k * LANES : (k + 1) * LANES]
            for y in range(2):
                target[y, z * channels : (z + 1) * channels, :] = parted(wide, y, channels)

    def view_slab(source, target):
        count = source.shape[0]
        part = source[...].astype(F32).reshape(2 * count, width)
        for k in range(width // LANES):
            wide[k, 0 : 2 * count, :] = part[:, k * LANES : (k + 1) * LANES]
        if count % 16 == 0:
            for z in range(2):
                target[z * count : (z + 1) * count, :] = parted(wide, z, count)
        else:
            target[...] = jnp.concatenate(
                [parted(wide, z, count).astype(F32) for z in range(2)], axis=0
            ).astype(BF16)

    loads[0].wait()
    slab(raw_vol, vol)
    loads[1].wait()
    bins = q_of(dot(mix, vol[0]), dot(mix, vol[1])).astype(BF16)
    spread(footprints(bins), tw, outbox.at[0])
    loads[2].wait()
    view_slab(raw_ds, ds)
    loads[3].wait()
    view_slab(raw_sino, sino)
    loads[4].wait()
    slab(raw_cvol, cvol)
    loads[5].wait()
    view_slab(raw_cd, cd)
    forward_weights(wdi, fdi, 48)
    forward_weights(wdo, fdo, 32)
    forward_weights(wpi, fpi, 48)
    forward_weights(wpo, fpo, 32)
    adjoint_weights(wpo, apo, 32)
    adjoint_weights(wpi, api, 48)
    adjoint_weights(wdo, ado, 32)
    adjoint_weights(wdi, adi, 48)
    pl.semaphore_wait(barrier, n - 1)
    exchange(outbox.at[0], inbox.at[0], 0)
    ds_copies = halo(ds, ds_h, OFFS, 0)
    si_copies = halo(sino, si_h, OFFS, 4)
    def fill_views(rows, own, others, first):
        for z in range(2):
            fill(rows, 2, z, first, own[z * channels : (z + 1) * channels, :])
        for slot, view in enumerate((0, 1, 3, 4)):
            for z in range(2):
                fill(rows, view, z, first, others[slot, z * channels : (z + 1) * channels, :])

    for copy in ds_copies:
        copy.wait_recv()
    fill_views(s_d, ds, ds_h, 0)
    for copy in si_copies:
        copy.wait_recv()

    all_of(inbox.at[0], 0).wait_recv()
    windows = gathered(inbox.at[0], pc, columns)
    pr_own[...] = jnp.concatenate(windows, axis=1).astype(BF16)
    pr_copies = halo(pr_own, pr_h, OFFS, 8)
    vol_copies = halo(vol, vol_h, (-1, 1), 12)
    cvol_copies = halo(cvol, cvol_h, (-1, 1), 14)

    def fill_tail(view, projected, measured):
        for z in range(2):
            block = jnp.concatenate(
                [
                    projected[z * 4 : z * 4 + 4].astype(F32),
                    measured[z * 4 : z * 4 + 4].astype(F32),
                    jnp.zeros((8, width), F32),
                ],
                axis=0,
            ).astype(BF16)
            fill(s_d, view, z, channels, block)

    fill_tail(2, pr_own[...], sino[...])
    for copy in pr_copies:
        copy.wait_recv()
    for slot, view in enumerate((0, 1, 3, 4)):
        fill_tail(view, pr_h[slot], si_h[slot])

    bias_di = column_of(bdi)

    @pl.loop(0, 3)
    def _(v):
        pre = dot(fdi[...], taken(s_d, v)) + bias_di
        dpre[v] = pre
        hidden = (pre * sigmoid(pre)).astype(BF16)
        for z in range(2):
            fill(s_dh, v, z, 0, hidden[z * channels : (z + 1) * channels])

    update = dot(fdo[...], taken(s_dh, 0)) + column_of(bdo)
    fresh = (ds[...].astype(F32) + update).astype(BF16)
    nd[...] = fresh
    stores[1].start()

    def bins_of(block, stride, first):
        return jnp.concatenate(
            [block[first : first + 4], block[stride + first : stride + first + 4]], axis=0
        )

    def parts_of(signal):
        return [signal[:, c * UW : (c + 1) * UW] for c in range(columns)]

    spread(parts_of(bins_of(fresh.astype(F32), channels, 0)), pc, outbox.at[1])
    exchange(outbox.at[1], inbox.at[1], 1)
    cd_copies = halo(cd, cd_h, OFFS, 16)

    low_in = jnp.where(me > 0, 1.0, 0.0).astype(F32)
    high_in = jnp.where(me < n - 1, 1.0, 0.0).astype(F32)

    def fill_rows(rows, own, others):
        for y in range(2):
            for z in range(2):
                part = slice(z * channels, (z + 1) * channels)
                fill(rows, 2 + y, z, 0, own[y, part, :])
                fill(rows, y, z, 0, (others[0, y, part, :].astype(F32) * low_in).astype(BF16))
                fill(rows, 4 + y, z, 0, (others[1, y, part, :].astype(F32) * high_in).astype(BF16))

    for copy in cvol_copies:
        copy.wait_recv()
    fill_rows(s_c, cvol, cvol_h)

    @pl.loop(0, 4)
    def _(r):
        hgrad[r] = dot(apo[...], taken(s_c, r))

    for copy in vol_copies:
        copy.wait_recv()
    fill_rows(s_p, vol, vol_h)

    all_of(inbox.at[1], 1).wait_recv()
    summed = tile_sums(gathered(inbox.at[1], tw, tables))
    bp_own[...] = summed.astype(BF16)
    bp_copies = halo(bp_own, bp_h, (-1, 1), 20)

    def fill_back(row, block):
        for z in range(2):
            part = jnp.concatenate(
                [block[z * 4 : z * 4 + 4], jnp.zeros((12, width), F32)], axis=0
            ).astype(BF16)
            fill(s_p, row, z, channels, part)

    own_back = bp_own[...].astype(F32)
    for y in range(2):
        fill_back(2 + y, own_back[:, y * width : (y + 1) * width])
    for copy in bp_copies:
        copy.wait_recv()
    low_back = bp_h[0].astype(F32) * low_in
    high_back = bp_h[1].astype(F32) * high_in
    for y in range(2):
        fill_back(y, low_back[:, y * width : (y + 1) * width])
        fill_back(4 + y, high_back[:, y * width : (y + 1) * width])

    bias_pi = column_of(bpi)

    @pl.loop(0, 4)
    def _(r):
        pre = dot(fpi[...], taken(s_p, r)) + bias_pi
        ppre[r] = pre
        inside = jnp.where(r == 0, low_in, jnp.where(r == 3, high_in, 1.0))
        s = sigmoid(pre)
        grad = (hgrad[r] * (s * (1.0 + pre * (1.0 - s))) * inside).astype(BF16)
        for z in range(2):
            fill(s_pg, r, z, 0, grad[z * channels : (z + 1) * channels])

    for r in range(2):
        ingrad[r] = dot(api[...], taken(s_pg, r))
    back = q_of(bins_of(ingrad[0], 48, channels), bins_of(ingrad[1], 48, channels)).astype(BF16)
    spread(footprints(back), tw, outbox.at[2])
    exchange(outbox.at[2], inbox.at[2], 2)

    @pl.loop(0, 4)
    def _(r):
        pre = ppre[r]
        inside = jnp.where(r == 0, low_in, jnp.where(r == 3, high_in, 1.0))
        hidden = (pre * sigmoid(pre) * inside).astype(BF16)
        for z in range(2):
            fill(s_ph, r, z, 0, hidden[z * channels : (z + 1) * channels])

    def packed(inner, outer, side):
        for k in range(9):
            rsum[k * 40 : (k + 1) * 40, :] = inner[k * 48 : k * 48 + 40]
        rsum[360:648, :] = outer
        lane = lax.broadcasted_iota(jnp.int32, (160, LANES), 1)
        tail = rsum[488:648, :]
        for i in range(3):
            moved = tail if i == 3 else pltpu.roll(tail, 96 - 32 * i, 1)
            pack[i * 160 : (i + 1) * 160, :] = jnp.where(
                lane < 96, rsum[i * 160 : (i + 1) * 160, :], moved
            )
        pack[480:488, :] = rsum[480:488, :]
        pack[488:512, :] = jnp.zeros((24, LANES), F32)
        px_out[side] = pack[pl.ds(other_half, 256), :].reshape(chips, chunk, LANES)
        return swap(px_out.at[side], px_in.at[side], 8 + side)

    own_half = pl.multiple_of(core * 256, 256)
    other_half = pl.multiple_of(256 - core * 256, 256)

    def chip_sum(side, copy):
        copy.wait_recv()
        own = pack[pl.ds(own_half, 256), :].reshape(chips, chunk, LANES)
        rs_out[side] = (own + px_in[side]).astype(BF16)

    def own_rows(rows, y):
        return jnp.concatenate([rows[y, 0, 1], rows[y, 1, 1]], axis=0)

    half_p = packed(
        weight_sum(s_p, 1, [own_rows(s_pg, 1), own_rows(s_pg, 2)]),
        weight_sum(s_ph, 0, [cvol[0], cvol[1]]),
        0,
    )
    for r in range(2):
        change = dot(fpo[...], taken(s_ph, r)) + column_of(bpo)
        nv[r] = (vol[r].astype(F32) + change).astype(BF16)
    stores[0].start()

    chip_sum(0, half_p)
    for copy in cd_copies:
        copy.wait_recv()

    def reduced(side):
        all_of(rs_in.at[side], 4 + side).wait_recv()

        def step(t, total):
            return total + rs_in[side, t].astype(F32)

        total = lax.fori_loop(0, chips, step, jnp.zeros((chunk, LANES), F32), unroll=4)
        ag_own[side] = total.astype(BF16)

    all_of(inbox.at[2], 2).wait_recv()
    toward = jnp.concatenate(gathered(inbox.at[2], pc, columns), axis=1)
    own_cot = cd[...].astype(F32)
    dtotal[...] = own_cot
    dtotal[0:4, :] = own_cot[0:4] + toward[0:4]
    dtotal[channels : channels + 4, :] = own_cot[channels : channels + 4] + toward[4:8]
    dc_own[...] = bins_of(dtotal[...], channels, 0).astype(BF16)
    dc_copies = halo(dc_own, dc_h, OFFS, 22)
    lanes(rs_out.at[0], rs_in.at[0], 4, False)
    own_total = dtotal[...].astype(BF16)
    for z in range(2):
        fill(s_dc, 2, z, 0, own_total[z * channels : (z + 1) * channels])
    for copy in dc_copies:
        copy.wait_recv()
    for slot, view in enumerate((0, 1, 3, 4)):
        for z in range(2):
            block = jnp.concatenate(
                [
                    dc_h[slot, z * 4 : z * 4 + 4, :].astype(F32),
                    cd_h[slot, z * channels + 4 : (z + 1) * channels, :].astype(F32),
                ],
                axis=0,
            ).astype(BF16)
            fill(s_dc, view, z, 0, block)

    @pl.loop(0, 3)
    def _(v):
        pre = dpre[v]
        s = sigmoid(pre)
        grad = (dot(ado[...], taken(s_dc, v)) * (s * (1.0 + pre * (1.0 - s)))).astype(BF16)
        for z in range(2):
            fill(s_dpg, v, z, 0, grad[z * channels : (z + 1) * channels])

    half_d = packed(
        weight_sum(s_d, 1, [own_rows(s_dpg, 1)]),
        weight_sum(s_dh, 0, [own_total]),
        1,
    )
    dhg[...] = dot(adi[...], taken(s_dpg, 0))
    spread(parts_of(bins_of(dhg[...], 48, channels).astype(BF16).astype(F32)), pc, outbox.at[3])
    chip_sum(1, half_d)
    lanes(rs_out.at[1], rs_in.at[1], 5, False)
    cut = 7 * ((n - 1) // 14)
    first_cut = 7 * ((n - 1) // 28)
    exchange(outbox.at[3], inbox.at[3], 3, 0, first_cut)
    for z in range(2):
        part = slice(z * channels, (z + 1) * channels)
        dg[part, :] = (dtotal[part, :] + dhg[z * 48 : z * 48 + channels, :]).astype(BF16)
    stores[3].start()
    reduced(0)
    class_far(ag_own.at[0], ag_in.at[0, core], 6)
    exchange(outbox.at[3], inbox.at[3], 3, first_cut, cut)
    reduced(1)
    lanes(ag_own.at[1], ag_in.at[1, core], 7, True)
    exchange(outbox.at[3], inbox.at[3], 3, cut, n - 1)
    all_of(ag_in.at[0, core], 6, members - 1).wait_recv()
    class_near(ag_in.at[0, core], 12)
    all_of(ag_in.at[0, core], 12, 3 * members).wait_recv()
    swaps = [swap(ag_in.at[0, core], ag_in.at[0, core], 10)]
    all_of(ag_in.at[1, core], 7).wait_recv()
    swaps.append(swap(ag_in.at[1, core], ag_in.at[1, core], 11))

    all_of(inbox.at[3], 3).wait_recv()
    final = tile_sums(gathered(inbox.at[3], tw, tables))
    high = final.astype(BF16)
    low = (final - high.astype(F32)).astype(BF16)
    both = jnp.concatenate([high.astype(F32), low.astype(F32)], axis=0).astype(BF16)
    for y in range(2):
        mixed = dot_tn(mix_twice, both[:, y * width : (y + 1) * width])
        for z in range(2):
            part = slice(z * channels, (z + 1) * channels)
            vg[y, part, :] = (
                cvol[y, part, :].astype(F32)
                + ingrad[y, z * 48 : z * 48 + channels, :]
                + mixed[part]
            ).astype(BF16)
    stores[2].start()

    for side, result in enumerate((gp, gd)):
        swaps[side].wait_recv()
        result[...] = ag_in[side].reshape(result.shape)

    for phase in range(4):
        all_of(inbox.at[phase], phase).wait_send()
    for side in range(2):
        all_of(rs_in.at[side], 4 + side).wait_send()
    all_of(ag_in.at[0, core], 6, members - 1).wait_send()
    all_of(ag_in.at[0, core], 12, 3 * members).wait_send()
    all_of(ag_in.at[1, core], 7).wait_send()
    for copy in halos:
        copy.wait_send()
    for copy in stores:
        copy.wait()


def finish(*refs):
    sources, targets, held, made = refs[:6], refs[6:14], refs[14:20], refs[20:28]
    wide, tall, load, store = refs[28:]
    loads = [pltpu.make_async_copy(a, b, load.at[i]) for i, (a, b) in enumerate(zip(sources, held))]
    stores = [pltpu.make_async_copy(a, b, store.at[i]) for i, (a, b) in enumerate(zip(made, targets))]
    for i in (4, 5, 0, 2, 1, 3):
        loads[i].start()
    channels = made[1].shape[0]
    width = made[1].shape[2]

    for side in range(2):
        loads[4 + side].wait()
        packed = held[4 + side]
        tall[0:488, :] = packed[0:488, :].astype(F32)
        lane = lax.broadcasted_iota(jnp.int32, (160, LANES), 1)
        rows = jnp.zeros((160, LANES), F32)
        for i in range(3):
            block = packed[i * 160 : (i + 1) * 160, :].astype(F32)
            rows = jnp.where(lane // 32 == i, pltpu.roll(block, 32 * (i + 1), 1), rows)
        tall[488:648, :] = rows
        tall[648:, :] = jnp.zeros((tall.shape[0] - 648, LANES), F32)
        flat = tall[...].T
        inner, outer = made[4 + 2 * side], made[5 + 2 * side]
        for i in range(3):
            part = flat[i * 32 : (i + 1) * 32]
            for k in range(9):
                inner[9 * i + k] = part[:, k * 40 : k * 40 + inner.shape[2]]
                outer[9 * i + k] = part[:, 360 + k * 32 : 360 + k * 32 + outer.shape[2]]
        stores[4 + 2 * side].start()
        stores[5 + 2 * side].start()

    for which in (0, 2):
        loads[which].wait()
        for z in range(2):
            for y in range(2):
                merged(wide, y, held[which][y, z * channels : (z + 1) * channels, :])
            made[which][:, z] = rows_from(wide).reshape(channels, 2, width).astype(BF16)
        stores[which].start()
    for which in (1, 3):
        loads[which].wait()
        for z in range(2):
            merged(wide, z, held[which][z * channels : (z + 1) * channels, :])
        made[which][...] = rows_from(wide).reshape(channels, 2, width).astype(BF16)
        stores[which].start()
    for copy in stores:
        copy.wait()


def shards(
    n,
    volume,
    dual_state,
    sinogram,
    cot_volume,
    cot_dual,
    basis_table,
    bin_energy,
    footprint_table,
    hit_tile,
    hit_table,
    hit_column,
    hit_count,
    primal_inner,
    primal_inner_bias,
    primal_outer,
    primal_outer_bias,
    dual_inner,
    dual_inner_bias,
    dual_outer,
    dual_outer_bias,
):
    channels, slices, row_count, width = volume.shape
    bin_count = sinogram.shape[0]
    columns = width // UW
    tables = footprint_table.shape[0]
    both = slices * channels

    chunk = 512 // n
    vmem = pl.BlockSpec(memory_space=pltpu.VMEM)
    smem = pl.BlockSpec(memory_space=pltpu.SMEM)
    shape = jax.ShapeDtypeStruct

    def rows_of(y, c):
        return pltpu.VMEM((y, 2, 3, c, width), BF16)

    any_space = pl.BlockSpec(memory_space=pl.ANY)
    messages = (n, slices * bin_count, UW)
    new_volume, new_dual, volume_grad, dual_grad, packed_primal, packed_dual = pl.pallas_call(
        functools.partial(kernel, n),
        out_shape=(
            shape((row_count, both, width), BF16),
            shape((both, width), BF16),
            shape((row_count, both, width), BF16),
            shape((both, width), BF16),
            shape((n * chunk, LANES), BF16),
            shape((n * chunk, LANES), BF16),
        ),
        in_specs=[smem] + [any_space] * 5 + [vmem, any_space] + [vmem] * 12,
        out_specs=(any_space,) * 4 + (vmem,) * 2,
        scratch_shapes=[
            pltpu.VMEM((row_count, both, width), BF16),
            pltpu.VMEM((both, width), BF16),
            pltpu.VMEM((row_count, both, width), BF16),
            pltpu.VMEM((both, width), BF16),
            pltpu.VMEM(volume.shape, BF16),
            pltpu.VMEM(volume.shape, BF16),
            pltpu.VMEM((channels, slices, width), BF16),
            pltpu.VMEM((channels, slices, width), BF16),
            pltpu.VMEM((bin_count, slices, width), BF16),
            pltpu.VMEM(footprint_table.shape, BF16),
            pltpu.VMEM((width // LANES, both, LANES), F32),
            pltpu.VMEM((row_count, both, width), BF16),
            pltpu.VMEM((row_count, both, width), BF16),
            pltpu.VMEM((both, width), BF16),
            pltpu.VMEM((both, width), BF16),
            pltpu.VMEM((slices * bin_count, width), BF16),
            pltpu.VMEM((tables, n, LANES), F32),
            pltpu.VMEM((columns, n, LANES), F32),
            pltpu.VMEM((64, 18 * 48), BF16),
            pltpu.VMEM((64, 18 * 32), BF16),
            pltpu.VMEM((64, 18 * 48), BF16),
            pltpu.VMEM((64, 18 * 32), BF16),
            pltpu.VMEM((96, 18 * 32), BF16),
            pltpu.VMEM((64, 18 * 32), BF16),
            pltpu.VMEM((96, 18 * 32), BF16),
            pltpu.VMEM((64, 18 * 32), BF16),
            rows_of(5, 48),
            rows_of(3, 32),
            rows_of(6, 48),
            rows_of(4, 32),
            rows_of(6, 32),
            rows_of(4, 32),
            rows_of(5, 32),
            rows_of(3, 32),
            pltpu.VMEM((4, both, width), BF16),
            pltpu.VMEM((4, 8, width), BF16),
            pltpu.VMEM((4, 8, width), BF16),
            pltpu.VMEM((2, row_count, both, width), BF16),
            pltpu.VMEM((2, row_count, both, width), BF16),
            pltpu.VMEM((4, both, width), BF16),
            pltpu.VMEM((2, 8, row_count * width), BF16),
            pltpu.VMEM((4, 8, width), BF16),
            pltpu.VMEM((8, width), BF16),
            pltpu.VMEM((8, row_count * width), BF16),
            pltpu.VMEM((8, width), BF16),
            pltpu.VMEM((3, both, width), F32),
            pltpu.VMEM((4, both, width), F32),
            pltpu.VMEM((4, both, width), F32),
            pltpu.VMEM((2, 96, width), F32),
            pltpu.VMEM((both, width), F32),
            pltpu.VMEM((96, width), F32),
            pltpu.VMEM((648, LANES), F32),
            pltpu.VMEM((512, LANES), F32),
            pltpu.VMEM((4,) + messages, BF16),
            pltpu.VMEM((4,) + messages, BF16),
            pltpu.VMEM((2, n // 2, chunk, LANES), F32),
            pltpu.VMEM((2, n // 2, chunk, LANES), F32),
            pltpu.VMEM((2, n // 2, chunk, LANES), BF16),
            pltpu.VMEM((2, n // 2, chunk, LANES), BF16),
            pltpu.VMEM((2, chunk, LANES), BF16),
            pltpu.VMEM((2, 2, n // 2, chunk, LANES), BF16),
            pltpu.SemaphoreType.DMA((10,)),
            pltpu.SemaphoreType.DMA((13,)),
            pltpu.SemaphoreType.DMA((13,)),
            pltpu.SemaphoreType.DMA((26,)),
            pltpu.SemaphoreType.DMA((26,)),
        ],
        compiler_params=pltpu.CompilerParams(
            collective_id=0, has_side_effects=True, vmem_limit_bytes=60 * 1024 * 1024
        ),
    )(
        bin_energy,
        volume,
        dual_state.reshape(channels, slices, width),
        sinogram.reshape(bin_count, slices, width),
        cot_volume,
        cot_dual.reshape(channels, slices, width),
        basis_table,
        footprint_table,
        hit_tile.T,
        hit_table.T,
        hit_column.T,
        hit_count.reshape(1, n),
        primal_inner,
        primal_outer,
        dual_inner,
        dual_outer,
        *(
            b.reshape(1, channels)
            for b in (primal_inner_bias, primal_outer_bias, dual_inner_bias, dual_outer_bias)
        ),
    )
    halves = (new_volume, new_dual, volume_grad, dual_grad, packed_primal, packed_dual)
    finals = (
        shape(volume.shape, BF16),
        shape((channels, slices, width), BF16),
        shape(volume.shape, BF16),
        shape((channels, slices, width), BF16),
        *(shape(w.shape, F32) for w in (primal_inner, primal_outer, dual_inner, dual_outer)),
    )
    new_volume, new_dual, volume_grad, dual_grad, *gradients = pl.pallas_call(
        finish,
        out_shape=finals,
        in_specs=[any_space] * 6,
        out_specs=(any_space,) * 8,
        scratch_shapes=[
            *(pltpu.VMEM(a.shape, a.dtype) for a in halves),
            *(pltpu.VMEM(a.shape, a.dtype) for a in finals),
            pltpu.VMEM((width // LANES, both, LANES), F32),
            pltpu.VMEM((768, LANES), F32),
            pltpu.SemaphoreType.DMA((6,)),
            pltpu.SemaphoreType.DMA((8,)),
        ],
    )(*halves)
    return (
        new_volume,
        new_dual.reshape(dual_state.shape),
        volume_grad,
        dual_grad.reshape(dual_state.shape),
        *gradients,
    )


def solution(mesh):
    part = P(None, "parts", AXIS, None)
    return jax.shard_map(
        functools.partial(shards, mesh.shape[AXIS]),
        mesh=mesh,
        in_specs=(part,) * 5 + (P(),) * 15,
        out_specs=(part,) * 4 + (P("parts", None, None),) * 4,
        check_vma=False,
    )
```
